256 devices in a mesh: dp: 32 (over x, z), cand: 8 (over y, core).
Axes of the slice: x: 4, y: 4, z: 8, core: 2. Of those that a mesh axis runs over, the one named last changes fastest.
Arguments:
- hidden: bfloat16 [64, 32, 128, 768], P('dp', 'cand'), may hold values from -24 to 24
- attn_weight: bfloat16 [768, 3072], P('dp'), may hold values from -1 to 1
- norm_gain: float32 [768], replicated, may hold values from 0.2 to 4
- pos_bias: float32 [12, 128, 128], replicated, may hold values from -5 to 5
- score_weight: float32 [768], replicated, may hold values from -4 to 4
- pair_lengths: int32 [64, 32], P('dp', 'cand'), may hold values from 32 to 128
- labels: int32 [64, 32], P('dp', 'cand'), may hold values from 0 to 3
Outputs:
- update: float32 [768, 3072], P('dp')
- loss: float32 [64], P('dp')
The draws below stay inside these ranges and needn't reach their ends.
All inputs are finite; a program needn't handle non-finite values.
Results may differ from the reference program's by a relative error of at most 0.017.
Values may be sent and summed in bfloat16 or wider, within the bound.
A program may use at most 128 MiB of HBM per device.

```python
import jax
import jax.numpy as jnp
from jax import lax

D = 768
HEADS = 12
HEAD = 64
SEQ = 128
CANDS = 32
QUERIES = 64


def draw_norm_gain(key, part):
    place = jnp.arange(D, dtype=jnp.int32).astype(jnp.float32) / jnp.float32(D)
    jitter = jax.random.uniform(jax.random.fold_in(key, 7401), (D,), jnp.float32, 0.75, 1.25)
    lowest, highest = (0.4, 2.0)
    values = jnp.exp(jnp.log(lowest) + (jnp.log(highest) - jnp.log(lowest)) * place) * jitter
    return jnp.clip(values, 0.2, 4.0)


def draw_score_weight(key, part):
    values = jax.random.normal(jax.random.fold_in(key, 7102), (D,), jnp.float32)
    values = jnp.clip(values, -6.0, 6.0) * jnp.sqrt(4.0 / jnp.float32(D))
    return jnp.clip(values, -4.0, 4.0)


def draw_attn_weight(key, part):
    values = jax.random.normal(jax.random.fold_in(key, 7301), (D, 4 * D), jnp.float32)
    values = jnp.clip(values, -6.0, 6.0) / jnp.sqrt(jnp.float32(D))
    column = jnp.arange(4 * D, dtype=jnp.int32)
    factor = jnp.where(column < D, 1.0 / jnp.sqrt(jnp.float32(HEAD)), 1.0)
    values = jnp.clip(values * factor[None, :], -1.0, 1.0)
    return values.astype(jnp.bfloat16)


def draw_hidden(key, part):
    normal_part = jax.random.normal(jax.random.fold_in(key, 7201), (QUERIES, CANDS, SEQ, D), jnp.float32)
    normal_part = jnp.clip(normal_part, -6.0, 6.0)
    values = normal_part
    return jnp.clip(values, -24.0, 24.0).astype(jnp.bfloat16)


def touch_ends(drawn, rng, least, largest):
    extent = drawn.shape
    index_at = [jax.random.randint(jax.random.fold_in(rng, axis), (), 0, extent[axis]) for axis in range(len(extent))]
    drawn = drawn.at[tuple(index_at)].set(least)
    longest = extent.index(max(extent))
    index_at[longest] = (index_at[longest] + 1) % extent[longest]
    return drawn.at[tuple(index_at)].set(largest)


def gaussian(stream_key, dims, scale, bound, kind=jnp.bfloat16):
    entries = jax.random.normal(stream_key, dims, jnp.float32) * scale
    return jnp.minimum(jnp.maximum(entries, -bound), bound).astype(kind)


def setup_inputs(seed: int = 0) -> dict:
    key_list = jax.random.split(jax.random.key(seed), 8)
    return {
        "hidden": draw_hidden(jax.random.fold_in(key_list[7], 71), 0),
        "attn_weight": draw_attn_weight(jax.random.fold_in(key_list[7], 71), 0),
        "norm_gain": draw_norm_gain(jax.random.fold_in(key_list[7], 71), 0),
        "pos_bias": gaussian(key_list[3], (HEADS, SEQ, SEQ), 1.0, 5.0, jnp.float32),
        "score_weight": draw_score_weight(jax.random.fold_in(key_list[7], 71), 0),
        "pair_lengths": touch_ends(jax.random.randint(key_list[5], (QUERIES, CANDS), SEQ // 4, SEQ + 1), jax.random.fold_in(key_list[5], 1), SEQ // 4, SEQ).astype(jnp.int32),
        "labels": touch_ends(jax.random.randint(key_list[6], (QUERIES, CANDS), 0, 4), jax.random.fold_in(key_list[6], 1), 0, 3).astype(jnp.int32),
    }


EPS = 1e-06

def rms_rows(values, gain):
    factor = lax.rsqrt(lax.optimization_barrier(jnp.mean(values * values, axis=-1, keepdims=True)) + EPS)
    return values * factor * gain

def attend(qkv, pos_bias, pair_len):
    batch, seq, triple = qkv.shape
    width = triple // 3
    heads = pos_bias.shape[0]
    head_size = width // heads
    parts = qkv.reshape(batch, seq, 3, heads, head_size).astype(jnp.float32)
    logits = jnp.einsum('bqhd,bkhd->bhqk', parts[:, :, 0], parts[:, :, 1])
    logits = logits + pos_bias[None]
    valid = jnp.arange(seq, dtype=jnp.int32)[None, :] < pair_len[:, None]
    logits = jnp.where(valid[:, None, None, :], logits, -1e+30)
    highest = lax.optimization_barrier(jnp.max(logits, axis=-1, keepdims=True))
    expo = jnp.exp(logits - highest)
    probs = (expo / lax.optimization_barrier(jnp.sum(expo, axis=-1, keepdims=True))).astype(jnp.bfloat16)
    context = jnp.einsum('bhqk,bkhd->bqhd', probs.astype(jnp.float32), parts[:, :, 2])
    return context.astype(jnp.bfloat16).reshape(batch, seq, width)

def forward(tokens, weights, norm_gain, pos_bias, pair_len):
    batch, seq, width = tokens.shape
    values = tokens.astype(jnp.float32)
    normed = rms_rows(values, norm_gain).astype(jnp.bfloat16)
    qkv = jnp.dot(normed.reshape(-1, width), weights[:, :3 * width], preferred_element_type=jnp.float32)
    qkv = qkv.astype(jnp.bfloat16).reshape(batch, seq, 3 * width)
    context = attend(qkv, pos_bias, pair_len)
    out_rows = values + jnp.dot(context.reshape(-1, width), weights[:, 3 * width:], preferred_element_type=jnp.float32).reshape(batch, seq, width)
    live = (jnp.arange(seq, dtype=jnp.int32)[None, :] < pair_len[:, None]).astype(jnp.float32)
    share = live / pair_len.astype(jnp.float32)[:, None]
    pooled = lax.optimization_barrier(jnp.sum(out_rows * share[:, :, None], axis=1))
    return (normed, qkv, context, pooled, share)

def score_head(pooled, score_weight):
    return lax.optimization_barrier(jnp.sum(rms_rows(pooled, 1.0) * score_weight, axis=-1))

def backward(normed, qkv, context, pooled, share, weights, pos_bias, pair_len, score_weight, score_grad):
    batch, seq, width = normed.shape
    unused, head_back = jax.vjp(lambda vector: score_head(vector, score_weight), pooled)
    pooled_grad = head_back(score_grad)[0]
    out_grad = (pooled_grad[:, None, :] * share[:, :, None]).astype(jnp.bfloat16)
    flat_out = out_grad.reshape(-1, width)
    context_grad = jnp.dot(flat_out, weights[:, 3 * width:].T, preferred_element_type=jnp.float32)
    context_grad = context_grad.astype(jnp.bfloat16).reshape(batch, seq, width)
    unused2, attend_back = jax.vjp(lambda block: attend(block, pos_bias, pair_len), qkv)
    qkv_grad = attend_back(context_grad)[0].reshape(-1, 3 * width)
    first = jnp.dot(normed.reshape(-1, width).T, qkv_grad, preferred_element_type=jnp.float32)
    second = jnp.dot(context.reshape(-1, width).T, flat_out, preferred_element_type=jnp.float32)
    return jnp.concatenate([first, second], axis=1)

def reference(hidden, attn_weight, norm_gain, pos_bias, score_weight, pair_lengths, labels):
    width = hidden.shape[3]

    def scores_of(pair):
        tokens, pair_len = pair
        unused_a, unused_b, unused_c, pooled, unused_d = forward(tokens, attn_weight, norm_gain, pos_bias, pair_len)
        return score_head(pooled, score_weight)
    scores = lax.map(scores_of, (hidden, pair_lengths))
    highest = lax.optimization_barrier(jnp.max(scores, axis=1, keepdims=True))
    expsum = lax.optimization_barrier(jnp.sum(jnp.exp(scores - highest), axis=1, keepdims=True))
    target = jnp.exp(labels.astype(jnp.float32))
    target_sum = lax.optimization_barrier(jnp.sum(target, axis=1, keepdims=True))
    target_dot = lax.optimization_barrier(jnp.sum(target * scores, axis=1, keepdims=True))
    loss = (highest + jnp.log(expsum) - target_dot / target_sum)[:, 0]
    score_grad = jnp.exp(scores - highest) / expsum - target / target_sum

    def accumulate(total, pair):
        tokens, pair_len, grad_row = pair
        normed, qkv, context, pooled, share = forward(tokens, attn_weight, norm_gain, pos_bias, pair_len)
        term = backward(normed, qkv, context, pooled, share, attn_weight, pos_bias, pair_len, score_weight, grad_row)
        return (total + term, None)
    start = jnp.zeros((width, 4 * width), jnp.float32)
    grad, unused = lax.scan(accumulate, start, (hidden, pair_lengths, score_grad))
    rms_value = jnp.sqrt(jnp.sum(grad * grad) / (4.0 * width * width))
    update = grad / (rms_value + EPS)
    return (update, loss)
```

```python
import functools

import jax
import jax.numpy as jnp
from jax import lax
from jax.experimental import pallas as pl
from jax.experimental.pallas import tpu as pltpu
from jax.sharding import Mesh
from jax.sharding import PartitionSpec as P

EPS = 1e-06
MESH = pl.DeviceIdType.MESH
F32, BF16 = jnp.float32, jnp.bfloat16
NEG = -1e30
PARTS = 3
LANES = 128


def dot(a, b, ca=1, cb=0):
    return lax.dot_general(a, b, (((ca,), (cb,)), ((), ())), preferred_element_type=F32)


def iota(shape, axis):
    return lax.broadcasted_iota(jnp.int32, shape, axis)


def step_kernel(dims, hid, wsh, gain, bias, sw, lens, labs, upd, loss, norm, norm_t, w, qk, prob, grad, hsum, svec, avec, uvec, dqk,
                zbuf, exb, r0, a1, a1s, b1, b1s, a2, b2, zs, z3, ob, sq,
                zsem, xsem, fsem, dsem, esem, r0sem, a1sem, b1sem, a2sem, b2sem, z3sem, obsem, sqsem):
    X, Z, Y, C = dims
    QL, CL, T, D = hid.shape
    H = bias.shape[0]
    HP = H // 2
    NP = QL * CL
    R = wsh.shape[0]
    XR = Z * R
    HR = XR // 2
    ZH = Z // 2
    NC = 4 * D // PARTS // C
    NB = NC // Y
    x, z, y, c = (lax.axis_index(name) for name in ("x", "z", "y", "c"))
    other = 1 - c
    cand = y * C + c
    started = []

    def at_x(d):
        return {"x": lax.rem(x + d, X)}

    def at_z(d):
        return {"z": lax.rem(z + d, Z)}

    def at_y(d):
        return {"y": lax.rem(y + d, Y)}

    def at_cand(i):
        return {"y": lax.rem(y + i // C, Y), "c": lax.rem(c + i % C, C)}

    def at_dp(i):
        return {"x": lax.rem(x + i // Z, X), "z": lax.rem(z + lax.rem(i, Z), Z)}

    def put(src, dst, sems, to):
        copy = pltpu.make_async_remote_copy(src, dst, sems.at[0], sems.at[1], device_id=to, device_id_type=MESH)
        copy.start()
        started.append(copy)
        return copy

    def cols(n, width):
        return pl.ds(pl.multiple_of(n, LANES), width)

    bar = pltpu.get_barrier_semaphore()

    def greet_dp(i, carry):
        pl.semaphore_signal(bar, 1, device_id=at_dp(i), device_id_type=MESH)
        return carry

    lax.fori_loop(1, X * Z, greet_dp, 0)
    for i in range(1, Y * C):
        pl.semaphore_signal(bar, 1, device_id=at_cand(i), device_id_type=MESH)

    def pair_len(p):
        return lens[p // CL, lax.rem(p, CL)]

    def normalise(p, carry):
        v = hid[p // CL, lax.rem(p, CL)].astype(F32)
        n = v * lax.rsqrt(jnp.mean(v * v, axis=1, keepdims=True) + EPS) * gain[...]
        rows = pl.ds(pl.multiple_of(p * T, T), T)
        norm[rows, :] = n.astype(BF16)
        norm_t[:, cols(p * T, T)] = n.T.astype(BF16)
        live = iota((T, 1), 0) < pair_len(p)
        hsum[pl.ds(p, 1), :] = jnp.sum(jnp.where(live, v, 0.0), axis=0, keepdims=True)
        return carry

    lax.fori_loop(0, NP, normalise, 0)
    pl.semaphore_wait(bar, X * Z - 1 + Y * C - 1)

    def part_cols(g, core):
        return cols((2 * g + core) * D, D)

    zcopies = {}
    for g in (0, 1):
        for d in range(1, Z):
            zcopies[g, d] = put(wsh.at[:, part_cols(g, c)], zbuf.at[g, z], zsem.at[g, d], at_z(d))
        zbuf[g, z] = wsh[:, part_cols(g, c)]

    def rows_of(d, lo=0, n=XR):
        return pl.ds(pl.multiple_of(lax.rem(x + d + X, X) * XR + lo, HR), n)

    near = [1] if X == 2 else [1, X - 1]
    xcopies, fcopies, dcopies = {}, {}, {}

    def gather_first(g):
        for d in range(1, Z):
            zcopies[g, d].wait_recv()
        for k in range(0, D, 256):
            blk = zbuf[g, :, :, k : k + 256].astype(F32).reshape(XR, 256).astype(BF16)
            w[rows_of(0), cols((2 * g + c) * D + k, 256)] = blk
        own = w.at[rows_of(0), part_cols(g, c)]
        for d in near:
            xcopies[g, d] = put(own, own, xsem.at[g, d], at_x(d))
        dcopies[g, 0] = put(own, own, dsem.at[g, 0], {"c": other})

    def gather_second(g):
        for d in near:
            xcopies[g, d].wait_recv()
            if X == 4:
                half = w.at[rows_of(-d, 0 if d == 1 else HR, HR), part_cols(g, c)]
                fcopies[g, d] = put(half, half, fsem.at[g, d], at_x(d))
            blk = w.at[rows_of(-d), part_cols(g, c)]
            dcopies[g, d] = put(blk, blk, dsem.at[g, d], {"c": other})

    def gather_third(g):
        if X == 4:
            for d in near:
                fcopies[g, d].wait_recv()
            blk = w.at[rows_of(2), part_cols(g, c)]
            dcopies[g, 2] = put(blk, blk, dsem.at[g, 2], {"c": other})

    def gather_last(g):
        for d in range(X):
            dcopies[g, d].wait_recv()

    gather_first(0)
    gather_second(0)
    gather_third(0)
    gather_first(1)
    gather_last(0)

    for n in range(0, 2 * D, 256):
        qk[:, n : n + 256] = dot(norm[...], w[:, n : n + 256]).astype(BF16)
    gather_second(1)

    half_lane = iota((1, LANES), 1) < LANES // 2
    ones = [jnp.where(half_lane, 1.0, 0.0).astype(BF16), jnp.where(half_lane, 0.0, 1.0).astype(BF16)]

    def both(v):
        return jnp.concatenate([v * ones[0], v * ones[1]], axis=0)

    svec[...] = jnp.zeros_like(svec)

    def attend(p, carry):
        rows = pl.ds(pl.multiple_of(p * T, T), T)
        n_live = pair_len(p)
        live_key = iota((1, T), 1) < n_live
        live_row = iota((T, 1), 0) < n_live
        for h in range(HP):
            q2 = qk[rows, h * LANES : (h + 1) * LANES]
            k2 = qk[rows, D + h * LANES : D + (h + 1) * LANES]
            s = dot(both(q2), k2, 1, 1) + bias[2 * h : 2 * h + 2].reshape(2 * T, T)
            s = jnp.where(live_key, s, NEG)
            e = jnp.exp(s - jnp.max(s, axis=1, keepdims=True))
            pr = (e * (1.0 / jnp.sum(e, axis=1, keepdims=True))).astype(BF16)
            prob[p, h] = pr
            for k in (0, 1):
                pk = jnp.where(live_row, pr[k * T : (k + 1) * T].astype(F32), 0.0)
                svec[p, 2 * h + k : 2 * h + k + 1, :] = jnp.sum(pk, axis=0, keepdims=True)
        a = dot(svec[p].astype(BF16), norm[rows, :])
        avec[pl.ds(pl.multiple_of(p * 16, 16), 16), :] = a.astype(BF16)
        return carry

    lax.fori_loop(0, NP, attend, 0)
    gather_third(1)
    gather_last(1)

    wv = w.at[:, 2 * D : 3 * D]
    wo = w.at[:, 3 * D : 4 * D]
    head_of = (iota((16, D), 1) // (D // H)) == iota((16, D), 0)
    prow = iota((NP, 1), 0)
    length, target = jnp.zeros((NP, 1), F32), jnp.zeros((NP, 1), F32)
    for p in range(NP):
        length = jnp.where(prow == p, lens[p // CL, p % CL].astype(F32), length)
        target = jnp.where(prow == p, labs[p // CL, p % CL].astype(F32), target)
    inv_len = 1.0 / length
    target = jnp.exp(target)

    zv = dot(avec[...], wv[...]).reshape(NP, 16, D)
    csum = jnp.sum(jnp.where(head_of[None], zv, 0.0), axis=1)
    pooled = hsum[...] * inv_len + dot((csum * inv_len).astype(BF16), wo[...])
    factor = lax.rsqrt(jnp.mean(pooled * pooled, axis=1, keepdims=True) + EPS)
    score = jnp.sum(pooled * factor * sw[...], axis=1, keepdims=True)

    exb[cand, 0] = jnp.broadcast_to(score, (NP, LANES))
    exb[cand, 1] = jnp.broadcast_to(target, (NP, LANES))
    ecopies = [put(exb.at[cand], exb.at[cand], esem.at[i], at_cand(i)) for i in range(1, Y * C)]
    for copy in ecopies:
        copy.wait_recv()
    scores, targets = exb[:, 0], exb[:, 1]
    query = iota((NP, LANES), 0) // CL

    def per_query(v, op, neutral):
        out = v
        for k in range(QL):
            out = jnp.where(query == k, op(jnp.where(query == k, v, neutral), axis=0, keepdims=True), out)
        return out

    highest = per_query(jnp.max(scores, axis=0), jnp.max, -jnp.inf)
    expsum = per_query(jnp.sum(jnp.exp(scores - highest[None]), axis=0), jnp.sum, 0.0)
    target_sum = per_query(jnp.sum(targets, axis=0), jnp.sum, 0.0)
    target_dot = per_query(jnp.sum(targets * scores, axis=0), jnp.sum, 0.0)
    loss[...] = highest + jnp.log(expsum) - target_dot / target_sum
    sgrad = (jnp.exp(score - highest) / expsum - target / target_sum)[:, :1]

    along = jnp.sum(pooled * sw[...], axis=1, keepdims=True) * (1.0 / D)
    pooled_grad = sgrad * (factor * sw[...] - pooled * (factor * factor * factor * along))
    g = (pooled_grad * inv_len).astype(BF16)
    cg = dot(g, wo[...], 1, 1)
    cexp = jnp.where(head_of[None], cg[:, None, :], 0.0).reshape(NP * 16, D).astype(BF16)
    tv = dot(cexp, wv[...], 1, 1).astype(BF16)
    for p in range(NP):
        uvec[p] = dot(tv[p * 16 : (p + 1) * 16], norm_t[:, p * T : (p + 1) * T])

    def keep(n, value):
        grad[:, :, n : n + value.shape[1]] = value.astype(BF16).reshape(X, XR, value.shape[1])

    csum_b = csum.astype(BF16)
    for n in range(0, D, 256):
        keep(n, dot(csum_b, g[:, n : n + 256], 0, 0))
    for n in range(0, D, 256):
        keep(D + n, dot(avec[...], cexp[:, n : n + 256], 0, 0))

    r0c, a1c, b1c, a2c, b2c, z3c, obc = {}, {}, {}, {}, {}, {}, {}

    def mine(t):
        return cols((t * C + c) * NC, NC)

    def reduce_0(t):
        r0c[t] = put(grad.at[:, :, cols((t * C + other) * NC, NC)], r0.at[t], r0sem.at[t], {"c": other})

    def reduce_1(t):
        r0c[t].wait_recv()
        r0[t] = (r0[t].astype(F32) + grad[:, :, mine(t)].astype(F32)).astype(BF16)
        for d in range(1, X):
            a1c[t, d] = put(r0.at[t, lax.rem(x + d, X), :HR, :], a1.at[t, d - 1], a1sem.at[t, d], at_x(d))
        for d in range(1, Y):
            to = cols(lax.rem(y + d, Y) * NB, NB)
            b1c[t, d] = put(r0.at[t, :, HR:, to], b1.at[t, d - 1], b1sem.at[t, d], at_y(d))

    def reduce_2(t):
        total = r0[t, x, :HR, :].astype(F32)
        for d in range(1, X):
            a1c[t, d].wait_recv()
            total += a1[t, d - 1].astype(F32)
        a1s[t] = total.astype(BF16)
        total = r0[t, :, HR:, cols(y * NB, NB)].astype(F32)
        for d in range(1, Y):
            b1c[t, d].wait_recv()
            total += b1[t, d - 1].astype(F32)
        b1s[t] = total.astype(BF16)
        for d in range(1, Y):
            a2c[t, d] = put(a1s.at[t, :, cols(lax.rem(y + d, Y) * NB, NB)], a2.at[t, d - 1], a2sem.at[t, d], at_y(d))
        for d in range(1, X):
            b2c[t, d] = put(b1s.at[t, lax.rem(x + d, X)], b2.at[t, d - 1], b2sem.at[t, d], at_x(d))

    def reduce_3(t):
        total = a1s[t, :, cols(y * NB, NB)].astype(F32)
        for d in range(1, Y):
            a2c[t, d].wait_recv()
            total += a2[t, d - 1].astype(F32)
        zs[t, :ZH] = total.reshape(ZH, R, NB).astype(BF16)
        total = b1s[t, x].astype(F32)
        for d in range(1, X):
            b2c[t, d].wait_recv()
            total += b2[t, d - 1].astype(F32)
        zs[t, ZH:] = total.reshape(ZH, R, NB).astype(BF16)
        for d in range(1, Z):
            z3c[t, d] = put(zs.at[t, lax.rem(z + d, Z)], z3.at[t, d - 1], z3sem.at[t, d], at_z(d))

    def reduce_4(t):
        total = zs[t, z].astype(F32)
        for d in range(1, Z):
            z3c[t, d].wait_recv()
            total += z3[t, d - 1].astype(F32)
        ob[t, cand] = total.astype(BF16)
        for i in range(1, Y * C):
            obc[t, i] = put(ob.at[t, cand], ob.at[t, cand], obsem.at[t, i], at_cand(i))

    def backward(h, carry):
        for p in range(NP):
            n_live = lens[p // CL, p % CL]
            live_row = iota((T, 1), 0) < n_live
            q2 = qk[p * T : (p + 1) * T, cols(h * LANES, LANES)]
            k2 = qk[p * T : (p + 1) * T, cols(D + h * LANES, LANES)]
            pr = prob[p, h].astype(F32).reshape(2, T, T)
            ds = []
            for k in (0, 1):
                pu = pr[k] * uvec[p, pl.ds(2 * h + k, 1), :]
                mean = jnp.sum(pu, axis=1, keepdims=True)
                ds.append(jnp.where(live_row, pu - pr[k] * mean, 0.0).astype(BF16))
            dqk[p * T : (p + 1) * T, :LANES] = dot(jnp.concatenate(ds, axis=1), both(k2)).astype(BF16)
            dqk[p * T : (p + 1) * T, LANES:] = dot(jnp.concatenate(ds, axis=0), both(q2), 0, 0).astype(BF16)
        dw = dot(norm_t[...], dqk[...]).astype(BF16)
        grad[:, :, cols(2 * D + h * 2 * LANES, 2 * LANES)] = dw.reshape(X, XR, 2 * LANES)
        return carry

    reduce_0(0)
    lax.fori_loop(0, 2, backward, 0)
    reduce_0(1)
    reduce_1(0)
    lax.fori_loop(2, 4, backward, 0)
    reduce_1(1)
    reduce_2(0)
    lax.fori_loop(4, HP, backward, 0)
    reduce_0(2)
    reduce_2(1)
    reduce_3(0)
    reduce_1(2)
    reduce_3(1)
    reduce_4(0)
    reduce_2(2)
    reduce_4(1)
    reduce_3(2)
    reduce_4(2)
    for copy in obc.values():
        copy.wait_recv()

    me = x * Z + z
    squares = jnp.zeros((R, NB), F32)
    for t in range(PARTS):
        for k in range(Y * C):
            v = ob[t, k].astype(F32)
            squares += v * v
    tile = squares.reshape(R // 8, 8, NB // LANES, LANES) if NB > LANES else squares.reshape(R // 8, 8, LANES)
    tile = jnp.sum(tile, axis=(0, 2)) if NB > LANES else jnp.sum(tile, axis=0)
    sq[me] = tile

    def sq_copy(i):
        return pltpu.make_async_remote_copy(
            sq.at[me], sq.at[me], sqsem.at[0, i], sqsem.at[1, i], device_id=at_dp(i), device_id_type=MESH
        )

    def sq_start(i, carry):
        sq_copy(i).start()
        return carry

    def sq_wait(i, carry):
        sq_copy(i).wait()
        return carry

    lax.fori_loop(1, X * Z, sq_start, 0)
    lax.fori_loop(1, X * Z, sq_wait, 0)
    everything = jnp.sum(sq[...], axis=0)
    everything = jnp.sum(jnp.sum(everything, axis=1, keepdims=True), axis=0, keepdims=True)
    scale = 1.0 / (jnp.sqrt(everything * (1.0 / (4.0 * D * D))) + EPS)
    for t in range(PARTS):
        for k in range(Y * C):
            for m in range(NB // LANES):
                b = ((t * C + k % C) * NC + (k // C) * NB) // LANES + m
                if b < HP:
                    n = 3 * D + b * LANES
                elif b < 2 * HP:
                    n = 2 * D + (b - HP) * LANES
                else:
                    n = (b - 2 * HP) % 2 * D + (b - 2 * HP) // 2 * LANES
                upd[:, n : n + LANES] = ob[t, k, :, m * LANES : (m + 1) * LANES].astype(F32) * scale
    for copy in started:
        copy.wait_send()


def solution(mesh):
    n_dp, n_cand = mesh.shape["dp"], mesh.shape["cand"]
    X, C = (4 if n_dp == 32 else 2), 2
    Z, Y = n_dp // X, n_cand // C
    split = Mesh(mesh.devices.reshape(X, Z, Y, C), ("x", "z", "y", "c"))
    dp, cand = ("x", "z"), ("y", "c")

    def shards(hidden, attn_weight, norm_gain, pos_bias, score_weight, pair_lengths, labels):
        QL, CL, T, D = hidden.shape
        H = pos_bias.shape[0]
        R = attn_weight.shape[0]
        NP, XR, NC = QL * CL, Z * R, 4 * D // PARTS // C
        HR, NB = XR // 2, NC // Y
        vmem, smem = pl.BlockSpec(memory_space=pltpu.VMEM), pl.BlockSpec(memory_space=pltpu.SMEM)
        dma = pltpu.SemaphoreType.DMA
        V = pltpu.VMEM
        update, loss = pl.pallas_call(
            functools.partial(step_kernel, (X, Z, Y, C)),
            out_shape=(jax.ShapeDtypeStruct((R, 4 * D), F32), jax.ShapeDtypeStruct((NP, LANES), F32)),
            in_specs=[vmem] * 5 + [smem] * 2,
            out_specs=(vmem, vmem),
            scratch_shapes=[
                V((NP * T, D), BF16),
                V((D, NP * T), BF16),
                V((D, 4 * D), BF16),
                V((NP * T, 2 * D), BF16),
                V((NP, H // 2, 2 * T, T), BF16),
                V((X, XR, 4 * D), BF16),
                V((NP, D), F32),
                V((NP, 16, T), F32),
                V((NP * 16, D), BF16),
                V((NP, 16, T), F32),
                V((NP * T, 2 * LANES), BF16),
                V((2, Z, R, D), BF16),
                V((Y * C, 2, NP, LANES), F32),
                V((PARTS, X, XR, NC), BF16),
                V((PARTS, X - 1, HR, NC), BF16),
                V((PARTS, HR, NC), BF16),
                V((PARTS, Y - 1, X, HR, NB), BF16),
                V((PARTS, X, HR, NB), BF16),
                V((PARTS, Y - 1, HR, NB), BF16),
                V((PARTS, X - 1, HR, NB), BF16),
                V((PARTS, Z, R, NB), BF16),
                V((PARTS, Z - 1, R, NB), BF16),
                V((PARTS, Y * C, R, NB), BF16),
                V((X * Z, 8, LANES), F32),
                dma((2, Z, 2)),
                dma((2, X, 2)),
                dma((2, X, 2)),
                dma((2, X, 2)),
                dma((Y * C, 2)),
                dma((PARTS, 2)),
                dma((PARTS, X, 2)),
                dma((PARTS, Y, 2)),
                dma((PARTS, Y, 2)),
                dma((PARTS, X, 2)),
                dma((PARTS, Z, 2)),
                dma((PARTS, Y * C, 2)),
                dma((2, X * Z)),
            ],
            compiler_params=pltpu.CompilerParams(collective_id=0, has_side_effects=True, vmem_limit_bytes=60 * 2**20),
        )(hidden, attn_weight, norm_gain[None], pos_bias, score_weight[None], pair_lengths, labels)
        return update, loss[::CL, 0]

    placed = (P(dp, cand, None, None), P(dp, None), P(), P(), P(), P(dp, cand), P(dp, cand))
    return jax.shard_map(shards, mesh=split, in_specs=placed, out_specs=(P(dp, None), P(dp)), check_vma=False)
```

```python
import functools

import jax
import jax.numpy as jnp
from jax import lax
from jax.experimental import pallas as pl
from jax.experimental.pallas import tpu as pltpu
from jax.sharding import Mesh
from jax.sharding import PartitionSpec as P

EPS = 1e-06
MESH = pl.DeviceIdType.MESH
F32, BF16 = jnp.float32, jnp.bfloat16
NEG = -1e30
PARTS = 3
LANES = 128


def dot(a, b, ca=1, cb=0):
    return lax.dot_general(a, b, (((ca,), (cb,)), ((), ())), preferred_element_type=F32)


def iota(shape, axis):
    return lax.broadcasted_iota(jnp.int32, shape, axis)


def step_kernel(dims, hid_in, wsh_in, gain, bias_in, sw, lens, labs, upd, loss, total_out, hid, wsh, bias, norm, norm_t, w, qk, prob, grad,
                hsum, svec, avec, uvec, dqk, zc, za, exb, r0, a0, b0, a1, a1s, b1, b1s, a2, b2, zs, z3, ob, sq,
                lsem, zsem, xsem, xfsem, ysem, yfsem, dsem, esem, r0sem, a0sem, b0sem, a1sem, b1sem, a2sem, b2sem, z3sem, obsem, sqsem):
    X, Z, Y, C = dims
    QL, CL, T, D = hid.shape
    H = bias.shape[0]
    HP = H // 2
    NP = QL * CL
    R = wsh.shape[0]
    XR = Z * R
    HR = XR // 2
    HQ = HR // 2
    ZH = Z // 2
    NC = 4 * D // PARTS // C
    NB = NC // Y
    x, z, y, c = (lax.axis_index(name) for name in ("x", "z", "y", "c"))
    other = 1 - c
    cand = y * C + c
    started = []

    def at_x(d):
        return {"x": lax.rem(x + d, X)}

    def at_z(d):
        return {"z": lax.rem(z + d, Z)}

    def at_y(d):
        return {"y": lax.rem(y + d, Y)}

    def at_cand(i):
        return {"y": lax.rem(y + i // C, Y), "c": lax.rem(c + i % C, C)}

    def at_dp(i):
        return {"x": lax.rem(x + i // Z, X), "z": lax.rem(z + lax.rem(i, Z), Z)}

    def put(src, dst, sems, to):
        copy = pltpu.make_async_remote_copy(src, dst, sems.at[0], sems.at[1], device_id=to, device_id_type=MESH)
        copy.start()
        started.append(copy)
        return copy

    def cols(n, width):
        return pl.ds(pl.multiple_of(n, LANES), width)

    loads = [pltpu.make_async_copy(src, dst, lsem.at[i]) for i, (src, dst) in enumerate(((hid_in, hid), (wsh_in, wsh), (bias_in, bias)))]
    for load in loads:
        load.start()

    near_x = [1] if X == 2 else [1, X - 1]
    near_y = [1] if Y == 2 else [1, Y - 1]
    first = [at_z(d) for d in range(1, Z)] + [at_x(d) for d in near_x] + [at_y(d) for d in near_y] + [{"c": other}]
    bar = pltpu.get_barrier_semaphore()
    for to in first:
        pl.semaphore_signal(bar, 1, device_id=to, device_id_type=MESH)

    def pair_len(p):
        return lens[p // CL, lax.rem(p, CL)]

    def normalise(p, carry):
        v = hid[p // CL, lax.rem(p, CL)].astype(F32)
        n = v * lax.rsqrt(jnp.mean(v * v, axis=1, keepdims=True) + EPS) * gain_row
        rows = pl.ds(pl.multiple_of(p * T, T), T)
        norm[rows, :] = n.astype(BF16)
        norm_t[:, cols(p * T, T)] = n.T.astype(BF16)
        live = iota((T, 1), 0) < pair_len(p)
        hsum[pl.ds(p, 1), :] = jnp.sum(jnp.where(live, v, 0.0), axis=0, keepdims=True)
        return carry

    gain_row, sw_row = gain[...].reshape(1, D), sw[...].reshape(1, D)
    loads[0].wait()
    lax.fori_loop(0, NP, normalise, 0)
    loads[1].wait()
    pl.semaphore_wait(bar, len(first))

    AW = D - Y * LANES
    wide = {"c": LANES, "a": AW}

    def wcols(g, core, kind, yy=0):
        base = (2 * g + core) * D
        return cols(base + yy * LANES, LANES) if kind == "c" else cols(base + Y * LANES, AW)

    def yrel(e):
        return lax.rem(y + e + Y, Y)

    def rows_of(d, lo=0, n=XR):
        return pl.ds(pl.multiple_of(lax.rem(x + d + X, X) * XR + lo, HR), n)

    zcopies, xcopies, xfcopies, ycopies, yfcopies, dcopies = {}, {}, {}, {}, {}, {}
    zbuf = {"c": zc, "a": za}
    kinds = ("c", "a")

    def z_start(g):
        for i, kind in enumerate(kinds):
            here = wcols(g, c, kind, y)
            for d in range(1, Z):
                zcopies[g, kind, d] = put(wsh.at[:, here], zbuf[kind].at[g, z], zsem.at[g, i, d], at_z(d))
            zbuf[kind][g, z] = wsh[:, here]

    def x_start(g, kind):
        i = kinds.index(kind)
        for d in range(1, Z):
            zcopies[g, kind, d].wait_recv()
        here = wcols(g, c, kind, y)
        w[rows_of(0), here] = zbuf[kind][g].astype(F32).reshape(XR, wide[kind]).astype(BF16)
        own = w.at[rows_of(0), here]
        for j, d in enumerate(near_x):
            xcopies[g, kind, d] = put(own, own, xsem.at[g, i, j], at_x(d))

    def x_forward(g, kind):
        i = kinds.index(kind)
        for j, d in enumerate(near_x):
            xcopies[g, kind, d].wait_recv()
            if X == 4:
                half = w.at[rows_of(-d, 0 if d == 1 else HR, HR), wcols(g, c, kind, y)]
                xfcopies[g, kind, d] = put(half, half, xfsem.at[g, i, j], at_x(d))

    def x_last(g, kind):
        if X == 4:
            for d in near_x:
                xfcopies[g, kind, d].wait_recv()

    def y_start(g, d):
        blk = w.at[rows_of(d), wcols(g, c, "c", y)]
        for j, e in enumerate(near_y):
            ycopies[g, d, e] = put(blk, blk, ysem.at[g, d, j], at_y(e))

    def y_forward(g, d):
        for j, e in enumerate(near_y):
            ycopies[g, d, e].wait_recv()
            if Y == 4:
                half = w.at[rows_of(d, 0 if e == 1 else HR, HR), wcols(g, c, "c", yrel(-e))]
                yfcopies[g, d, e] = put(half, half, yfsem.at[g, d, j], at_y(e))

    def y_last(g):
        if Y == 4:
            for d in range(X):
                for e in near_y:
                    yfcopies[g, d, e].wait_recv()

    def hand_over(g, k, kind, yy=0):
        blk = w.at[:, wcols(g, c, kind, yy)]
        dcopies[g, k] = put(blk, blk, dsem.at[g, k], {"c": other})

    def hand_near(g):
        for e in near_y:
            hand_over(g, 1 + e, "c", yrel(e))

    def hand_last(g):
        y_last(g)
        if Y == 4:
            hand_over(g, 3, "c", yrel(2))

    def taken(g):
        for key, copy in dcopies.items():
            if key[0] == g:
                copy.wait_recv()

    z_start(0)
    z_start(1)
    x_start(0, "c")
    y_start(0, 0)
    x_start(0, "a")
    x_forward(0, "c")
    for d in near_x:
        y_start(0, d)
    y_forward(0, 0)
    x_forward(0, "a")
    x_last(0, "c")
    if X == 4:
        y_start(0, 2)
    hand_over(0, 1, "c", y)
    for d in near_x:
        y_forward(0, d)
    x_last(0, "a")
    hand_over(0, 0, "a")
    x_start(1, "c")
    x_start(1, "a")
    if X == 4:
        y_forward(0, 2)
    hand_near(0)
    y_start(1, 0)
    hand_last(0)
    x_forward(1, "c")
    for d in near_x:
        y_start(1, d)
    x_forward(1, "a")
    taken(0)

    for n in range(0, 2 * D, 256):
        qk[:, n : n + 256] = dot(norm[...], w[:, n : n + 256]).astype(BF16)
    loads[2].wait()
    y_forward(1, 0)
    x_last(1, "c")
    if X == 4:
        y_start(1, 2)
    hand_over(1, 1, "c", y)
    x_last(1, "a")
    hand_over(1, 0, "a")

    half_lane = iota((1, LANES), 1) < LANES // 2
    ones = [jnp.where(half_lane, 1.0, 0.0).astype(BF16), jnp.where(half_lane, 0.0, 1.0).astype(BF16)]

    def both(v):
        return jnp.concatenate([v * ones[0], v * ones[1]], axis=0)

    svec[...] = jnp.zeros_like(svec)

    def attend(p, carry):
        rows = pl.ds(pl.multiple_of(p * T, T), T)
        n_live = pair_len(p)
        live_key = iota((1, T), 1) < n_live
        live_row = iota((T, 1), 0) < n_live
        for h in range(HP):
            q2 = qk[rows, h * LANES : (h + 1) * LANES]
            k2 = qk[rows, D + h * LANES : D + (h + 1) * LANES]
            s = dot(both(q2), k2, 1, 1) + bias[2 * h : 2 * h + 2].reshape(2 * T, T)
            s = jnp.where(live_key, s, NEG)
            e = jnp.exp(s - jnp.max(s, axis=1, keepdims=True))
            pr = (e * (1.0 / jnp.sum(e, axis=1, keepdims=True))).astype(BF16)
            prob[p, h] = pr
            for k in (0, 1):
                pk = jnp.where(live_row, pr[k * T : (k + 1) * T].astype(F32), 0.0)
                svec[p, 2 * h + k : 2 * h + k + 1, :] = jnp.sum(pk, axis=0, keepdims=True)
        a = dot(svec[p].astype(BF16), norm[rows, :])
        avec[pl.ds(pl.multiple_of(p * 16, 16), 16), :] = a.astype(BF16)
        return carry

    lax.fori_loop(0, NP // 2, attend, 0)
    for d in range(1, X):
        y_forward(1, d)
    hand_near(1)
    lax.fori_loop(NP // 2, NP, attend, 0)
    hand_last(1)
    taken(1)

    wv = w.at[:, 2 * D : 3 * D]
    wo = w.at[:, 3 * D : 4 * D]
    head_of = (iota((16, D), 1) // (D // H)) == iota((16, D), 0)
    prow = iota((NP, 1), 0)
    length, target = jnp.zeros((NP, 1), F32), jnp.zeros((NP, 1), F32)
    for p in range(NP):
        length = jnp.where(prow == p, lens[p // CL, p % CL].astype(F32), length)
        target = jnp.where(prow == p, labs[p // CL, p % CL].astype(F32), target)
    inv_len = 1.0 / length
    target = jnp.exp(target)

    zv = dot(avec[...], wv[...]).reshape(NP, 16, D)
    csum = jnp.sum(jnp.where(head_of[None], zv, 0.0), axis=1)
    pooled = hsum[...] * inv_len + dot((csum * inv_len).astype(BF16), wo[...])
    factor = lax.rsqrt(jnp.mean(pooled * pooled, axis=1, keepdims=True) + EPS)
    score = jnp.sum(pooled * factor * sw_row, axis=1, keepdims=True)

    exb[cand, 0] = jnp.broadcast_to(score, (NP, LANES))
    exb[cand, 1] = jnp.broadcast_to(target, (NP, LANES))
    ecopies = [put(exb.at[cand], exb.at[cand], esem.at[i], at_cand(i)) for i in range(1, Y * C)]
    for copy in ecopies:
        copy.wait_recv()
    scores, targets = exb[:, 0], exb[:, 1]
    query = iota((NP, LANES), 0) // CL

    def per_query(v, op, neutral):
        out = v
        for k in range(QL):
            out = jnp.where(query == k, op(jnp.where(query == k, v, neutral), axis=0, keepdims=True), out)
        return out

    highest = per_query(jnp.max(scores, axis=0), jnp.max, -jnp.inf)
    expsum = per_query(jnp.sum(jnp.exp(scores - highest[None]), axis=0), jnp.sum, 0.0)
    target_sum = per_query(jnp.sum(targets, axis=0), jnp.sum, 0.0)
    target_dot = per_query(jnp.sum(targets * scores, axis=0), jnp.sum, 0.0)
    losses = highest + jnp.log(expsum) - target_dot / target_sum
    for k in range(QL):
        loss[k] = jnp.max(losses[k * CL : k * CL + 1])
    sgrad = (jnp.exp(score - highest) / expsum - target / target_sum)[:, :1]

    along = jnp.sum(pooled * sw_row, axis=1, keepdims=True) * (1.0 / D)
    pooled_grad = sgrad * (factor * sw_row - pooled * (factor * factor * factor * along))
    g = (pooled_grad * inv_len).astype(BF16)
    cg = dot(g, wo[...], 1, 1)
    cexp = jnp.where(head_of[None], cg[:, None, :], 0.0).reshape(NP * 16, D).astype(BF16)
    tv = dot(cexp, wv[...], 1, 1).astype(BF16)
    for p in range(NP):
        uvec[p] = dot(tv[p * 16 : (p + 1) * 16], norm_t[:, p * T : (p + 1) * T])

    def keep(n, value):
        grad[:, :, n : n + value.shape[1]] = value.astype(BF16).reshape(X, XR, value.shape[1])

    csum_b = csum.astype(BF16)
    for n in range(0, D, 256):
        keep(n, dot(csum_b, g[:, n : n + 256], 0, 0))
    for n in range(0, D, 256):
        keep(D + n, dot(avec[...], cexp[:, n : n + 256], 0, 0))

    a0c, b0c, r0c, a1c, b1c, a2c, b2c, z3c, obc = {}, {}, {}, {}, {}, {}, {}, {}, {}

    def mine(t):
        return cols((t * C + c) * NC, NC)

    def reduce_0(t):
        r0c[t] = put(grad.at[:, :, cols((t * C + other) * NC, NC)], r0.at[t], r0sem.at[t], {"c": other})

    def reduce_1(t):
        r0c[t].wait_recv()
        r0[t] = (r0[t].astype(F32) + grad[:, :, mine(t)].astype(F32)).astype(BF16)
        if X == 4:
            far = lax.rem(x + 2, X)
            for j, d in enumerate(near_x):
                a0c[t, j] = put(r0.at[t, far, j * HQ : (j + 1) * HQ, :], a0.at[t, j], a0sem.at[t, j], at_x(d))
        if Y == 4:
            far = cols(yrel(2) * NB, NB)
            for j, e in enumerate(near_y):
                b0c[t, j] = put(r0.at[t, :, HR + j * HQ : HR + (j + 1) * HQ, far], b0.at[t, j], b0sem.at[t, j], at_y(e))

    def reduce_1b(t):
        for j, d in enumerate(near_x):
            ahead = lax.rem(x + d, X)
            if X == 4:
                a0c[t, j].wait_recv()
                part = pl.ds(j * HQ, HQ)
                r0[t, ahead, part, :] = (r0[t, ahead, part, :].astype(F32) + a0[t, j].astype(F32)).astype(BF16)
            a1c[t, j] = put(r0.at[t, ahead, :HR, :], a1.at[t, j], a1sem.at[t, j], at_x(d))
        for j, e in enumerate(near_y):
            ahead = cols(yrel(e) * NB, NB)
            if Y == 4:
                b0c[t, j].wait_recv()
                part = pl.ds(HR + j * HQ, HQ)
                r0[t, :, part, ahead] = (r0[t, :, part, ahead].astype(F32) + b0[t, j].astype(F32)).astype(BF16)
            b1c[t, j] = put(r0.at[t, :, HR:, ahead], b1.at[t, j], b1sem.at[t, j], at_y(e))

    def reduce_2(t):
        total = r0[t, x, :HR, :].astype(F32)
        for j in range(len(near_x)):
            a1c[t, j].wait_recv()
            total += a1[t, j].astype(F32)
        a1s[t] = total.astype(BF16)
        total = r0[t, :, HR:, cols(y * NB, NB)].astype(F32)
        for j in range(len(near_y)):
            b1c[t, j].wait_recv()
            total += b1[t, j].astype(F32)
        b1s[t] = total.astype(BF16)
        for d in range(1, Y):
            a2c[t, d] = put(a1s.at[t, :, cols(lax.rem(y + d, Y) * NB, NB)], a2.at[t, d - 1], a2sem.at[t, d], at_y(d))
        for d in range(1, X):
            b2c[t, d] = put(b1s.at[t, lax.rem(x + d, X)], b2.at[t, d - 1], b2sem.at[t, d], at_x(d))

    def reduce_3(t):
        total = a1s[t, :, cols(y * NB, NB)].astype(F32)
        for d in range(1, Y):
            a2c[t, d].wait_recv()
            total += a2[t, d - 1].astype(F32)
        zs[t, :ZH] = total.reshape(ZH, R, NB).astype(BF16)
        total = b1s[t, x].astype(F32)
        for d in range(1, X):
            b2c[t, d].wait_recv()
            total += b2[t, d - 1].astype(F32)
        zs[t, ZH:] = total.reshape(ZH, R, NB).astype(BF16)
        for d in range(1, Z):
            z3c[t, d] = put(zs.at[t, lax.rem(z + d, Z)], z3.at[t, d - 1], z3sem.at[t, d], at_z(d))

    def reduce_4(t):
        total = zs[t, z].astype(F32)
        for d in range(1, Z):
            z3c[t, d].wait_recv()
            total += z3[t, d - 1].astype(F32)
        ob[t, cand] = total.astype(BF16)
        for i in range(1, Y * C):
            obc[t, i] = put(ob.at[t, cand], ob.at[t, cand], obsem.at[t, i], at_cand(i))

    def backward(h, carry):
        for p in range(NP):
            n_live = lens[p // CL, p % CL]
            live_row = iota((T, 1), 0) < n_live
            q2 = qk[p * T : (p + 1) * T, cols(h * LANES, LANES)]
            k2 = qk[p * T : (p + 1) * T, cols(D + h * LANES, LANES)]
            pr = prob[p, h].astype(F32).reshape(2, T, T)
            ds = []
            for k in (0, 1):
                pu = pr[k] * uvec[p, pl.ds(2 * h + k, 1), :]
                mean = jnp.sum(pu, axis=1, keepdims=True)
                ds.append(jnp.where(live_row, pu - pr[k] * mean, 0.0).astype(BF16))
            dqk[p * T : (p + 1) * T, :LANES] = dot(jnp.concatenate(ds, axis=1), both(k2)).astype(BF16)
            dqk[p * T : (p + 1) * T, LANES:] = dot(jnp.concatenate(ds, axis=0), both(q2), 0, 0).astype(BF16)
        dw = dot(norm_t[...], dqk[...]).astype(BF16)
        grad[:, :, cols(2 * D + h * 2 * LANES, 2 * LANES)] = dw.reshape(X, XR, 2 * LANES)
        return carry

    reduce_0(0)
    lax.fori_loop(0, 2, backward, 0)
    reduce_0(1)
    reduce_1(0)
    lax.fori_loop(2, 4, backward, 0)
    reduce_1b(0)
    reduce_1(1)
    lax.fori_loop(4, HP, backward, 0)
    reduce_0(2)
    reduce_2(0)
    reduce_1b(1)
    reduce_1(2)
    reduce_3(0)
    reduce_2(1)
    reduce_1b(2)
    reduce_3(1)
    reduce_4(0)
    reduce_2(2)
    reduce_4(1)
    reduce_3(2)
    reduce_4(2)
    for copy in obc.values():
        copy.wait_recv()

    me = x * Z + z
    squares = jnp.zeros((R, NB), F32)
    for t in range(PARTS):
        for k in range(Y * C):
            v = ob[t, k].astype(F32)
            squares += v * v
    tile = squares.reshape(R // 8, 8, NB // LANES, LANES) if NB > LANES else squares.reshape(R // 8, 8, LANES)
    tile = jnp.sum(tile, axis=(0, 2)) if NB > LANES else jnp.sum(tile, axis=0)
    sq[me] = tile

    def sq_copy(i):
        return pltpu.make_async_remote_copy(
            sq.at[me], sq.at[me], sqsem.at[0, i], sqsem.at[1, i], device_id=at_dp(i), device_id_type=MESH
        )

    def sq_start(i, carry):
        sq_copy(i).start()
        return carry

    def sq_wait(i, carry):
        sq_copy(i).wait()
        return carry

    lax.fori_loop(1, X * Z, sq_start, 0)
    for t in range(PARTS):
        for k in range(Y * C):
            for m in range(NB // LANES):
                b = ((t * C + k % C) * NC + (k // C) * NB) // LANES + m
                if b < HP:
                    n = 3 * D + b * LANES
                elif b < 2 * HP:
                    n = 2 * D + (b - HP) * LANES
                else:
                    n = (b - 2 * HP) % 2 * D + (b - 2 * HP) // 2 * LANES
                upd[:, n : n + LANES] = ob[t, k, :, m * LANES : (m + 1) * LANES]
    lax.fori_loop(1, X * Z, sq_wait, 0)
    total_out[0] = jnp.sum(sq[...])
    for copy in started:
        copy.wait_send()


def solution(mesh):
    n_dp, n_cand = mesh.shape["dp"], mesh.shape["cand"]
    X, C = (4 if n_dp == 32 else 2), 2
    Z, Y = n_dp // X, n_cand // C
    split = Mesh(mesh.devices.reshape(X, Z, Y, C), ("x", "z", "y", "c"))
    dp, cand = ("x", "z"), ("y", "c")

    def shards(hidden, attn_weight, norm_gain, pos_bias, score_weight, pair_lengths, labels):
        QL, CL, T, D = hidden.shape
        H = pos_bias.shape[0]
        R = attn_weight.shape[0]
        NP, XR, NC = QL * CL, Z * R, 4 * D // PARTS // C
        HR, NB = XR // 2, NC // Y
        hbm = pl.BlockSpec(memory_space=pl.ANY)
        vmem, smem = pl.BlockSpec(memory_space=pltpu.VMEM), pl.BlockSpec(memory_space=pltpu.SMEM)
        dma = pltpu.SemaphoreType.DMA
        V = pltpu.VMEM
        summed, loss, squares = pl.pallas_call(
            functools.partial(step_kernel, (X, Z, Y, C)),
            out_shape=(
                jax.ShapeDtypeStruct((R, 4 * D), BF16),
                jax.ShapeDtypeStruct((QL,), F32),
                jax.ShapeDtypeStruct((1,), F32),
            ),
            in_specs=[hbm, hbm, vmem, hbm, vmem, smem, smem],
            out_specs=(vmem, smem, smem),
            scratch_shapes=[
                V(hidden.shape, BF16),
                V(attn_weight.shape, BF16),
                V(pos_bias.shape, F32),
                V((NP * T, D), BF16),
                V((D, NP * T), BF16),
                V((D, 4 * D), BF16),
                V((NP * T, 2 * D), BF16),
                V((NP, H // 2, 2 * T, T), BF16),
                V((X, XR, 4 * D), BF16),
                V((NP, D), F32),
                V((NP, 16, T), F32),
                V((NP * 16, D), BF16),
                V((NP, 16, T), F32),
                V((NP * T, 2 * LANES), BF16),
                V((2, Z, R, LANES), BF16),
                V((2, Z, R, D - Y * LANES), BF16),
                V((Y * C, 2, NP, LANES), F32),
                V((PARTS, X, XR, NC), BF16),
                V((PARTS, 2, HR // 2, NC), BF16),
                V((PARTS, 2, X, HR // 2, NB), BF16),
                V((PARTS, 2, HR, NC), BF16),
                V((PARTS, HR, NC), BF16),
                V((PARTS, 2, X, HR, NB), BF16),
                V((PARTS, X, HR, NB), BF16),
                V((PARTS, Y - 1, HR, NB), BF16),
                V((PARTS, X - 1, HR, NB), BF16),
                V((PARTS, Z, R, NB), BF16),
                V((PARTS, Z - 1, R, NB), BF16),
                V((PARTS, Y * C, R, NB), BF16),
                V((X * Z, 8, LANES), F32),
                dma((3,)),
                dma((2, 2, Z, 2)),
                dma((2, 2, 2, 2)),
                dma((2, 2, 2, 2)),
                dma((2, X, 2, 2)),
                dma((2, X, 2, 2)),
                dma((2, 1 + Y, 2)),
                dma((Y * C, 2)),
                dma((PARTS, 2)),
                dma((PARTS, 2, 2)),
                dma((PARTS, 2, 2)),
                dma((PARTS, 2, 2)),
                dma((PARTS, 2, 2)),
                dma((PARTS, Y, 2)),
                dma((PARTS, X, 2)),
                dma((PARTS, Z, 2)),
                dma((PARTS, Y * C, 2)),
                dma((2, X * Z)),
            ],
            compiler_params=pltpu.CompilerParams(collective_id=0, has_side_effects=True, vmem_limit_bytes=60 * 2**20),
        )(hidden, attn_weight, norm_gain, pos_bias, score_weight, pair_lengths, labels)
        scale = 1.0 / (jnp.sqrt(squares[0] / (4.0 * D * D)) + EPS)
        return summed.astype(F32) * scale, loss

    placed = (P(dp, cand, None, None), P(dp, None), P(), P(), P(), P(dp, cand), P(dp, cand))
    return jax.shard_map(shards, mesh=split, in_specs=placed, out_specs=(P(dp, None), P(dp)), check_vma=False)
```

```python
import functools

import jax
import jax.numpy as jnp
from jax import lax
from jax.experimental import pallas as pl
from jax.experimental.pallas import tpu as pltpu
from jax.sharding import Mesh
from jax.sharding import PartitionSpec as P

EPS = 1e-06
MESH = pl.DeviceIdType.MESH
F32, BF16 = jnp.float32, jnp.bfloat16
NEG = -1e30
PARTS = 3
LANES = 128


def dot(a, b, ca=1, cb=0):
    return lax.dot_general(a, b, (((ca,), (cb,)), ((), ())), preferred_element_type=F32)


def iota(shape, axis):
    return lax.broadcasted_iota(jnp.int32, shape, axis)


def step_kernel(dims, hid_in, wsh_in, gain, bias_in, sw, lens, labs, upd, loss, total_out, hid, wsh, bias, norm, norm_t, w, qk, prob, grad,
                hsum, svec, avec, uvec, dqk, dsend, mixed, zc, za, exb, a0, b0, a1, a1s, b1, b1s, a2, b2, zs, z3, ob, sqz, sq,
                lsem, zsem, xsem, xfsem, ysem, yfsem, dsem, psem, qsem, esem, a0sem, b0sem, a1sem, b1sem, a2sem, b2sem, z3sem, obsem,
                sqzsem, sqsem):
    X, Z, Y, C = dims
    QL, CL, T, D = hid.shape
    H = bias.shape[0]
    HP = H // 2
    HC = HP // C
    DC = D // C
    NP = QL * CL
    R = wsh.shape[0]
    XR = Z * R
    HR = XR // 2
    HQ = HR // 2
    ZH = Z // 2
    NC = 4 * D // PARTS // C
    NB = NC // Y
    x, z, y, c = (lax.axis_index(name) for name in ("x", "z", "y", "c"))
    other = 1 - c
    cand = y * C + c
    started = []

    def at_x(d):
        return {"x": lax.rem(x + d, X)}

    def at_z(d):
        return {"z": lax.rem(z + d, Z)}

    def at_y(d):
        return {"y": lax.rem(y + d, Y)}

    def at_cand(i):
        return {"y": lax.rem(y + i // C, Y), "c": lax.rem(c + i % C, C)}

    def put(src, dst, sems, to):
        copy = pltpu.make_async_remote_copy(src, dst, sems.at[0], sems.at[1], device_id=to, device_id_type=MESH)
        copy.start()
        started.append(copy)
        return copy

    def cols(n, width):
        return pl.ds(pl.multiple_of(n, LANES), width)

    loads = [pltpu.make_async_copy(src, dst, lsem.at[i]) for i, (src, dst) in enumerate(((hid_in, hid), (wsh_in, wsh), (bias_in, bias)))]
    for load in loads:
        load.start()

    near_x = [1] if X == 2 else [1, X - 1]
    near_y = [1] if Y == 2 else [1, Y - 1]
    first = [at_z(d) for d in range(1, Z)] + [at_x(d) for d in near_x] + [at_y(d) for d in near_y] + [{"c": other}]
    bar = pltpu.get_barrier_semaphore()
    for to in first:
        pl.semaphore_signal(bar, 1, device_id=to, device_id_type=MESH)

    def pair_len(p):
        return lens[p // CL, lax.rem(p, CL)]

    def normalise(p, carry):
        v = hid[p // CL, lax.rem(p, CL)].astype(F32)
        n = v * lax.rsqrt(jnp.mean(v * v, axis=1, keepdims=True) + EPS) * gain_row
        rows = pl.ds(pl.multiple_of(p * T, T), T)
        norm[rows, :] = n.astype(BF16)
        norm_t[c, :, cols(p * T, T)] = n.T.astype(BF16)
        live = iota((T, 1), 0) < pair_len(p)
        hsum[pl.ds(p, 1), :] = jnp.sum(jnp.where(live, v, 0.0), axis=0, keepdims=True)
        return carry

    gain_row, sw_row = gain[...].reshape(1, D), sw[...].reshape(1, D)
    loads[0].wait()
    lax.fori_loop(0, NP, normalise, 0)
    loads[1].wait()
    pl.semaphore_wait(bar, len(first))

    def swap(ref, sem):
        return put(ref, ref, sem, {"c": other})

    norm_copy = swap(norm_t.at[c], psem.at[0])

    AW = D - Y * LANES
    wide = {"c": LANES, "a": AW}

    def wcols(g, core, kind, yy=0):
        base = (2 * g + core) * D
        return cols(base + yy * LANES, LANES) if kind == "c" else cols(base + Y * LANES, AW)

    def yrel(e):
        return lax.rem(y + e + Y, Y)

    def rows_of(d, lo=0, n=XR):
        return pl.ds(pl.multiple_of(lax.rem(x + d + X, X) * XR + lo, HR), n)

    zcopies, xcopies, xfcopies, ycopies, yfcopies, dcopies = {}, {}, {}, {}, {}, {}
    zbuf = {"c": zc, "a": za}
    kinds = ("c", "a")

    def z_start(g):
        for i, kind in enumerate(kinds):
            here = wcols(g, c, kind, y)
            for d in range(1, Z):
                zcopies[g, kind, d] = put(wsh.at[:, here], zbuf[kind].at[g, z], zsem.at[g, i, d], at_z(d))
            zbuf[kind][g, z] = wsh[:, here]

    def x_start(g, kind):
        i = kinds.index(kind)
        for d in range(1, Z):
            zcopies[g, kind, d].wait_recv()
        here = wcols(g, c, kind, y)
        w[rows_of(0), here] = zbuf[kind][g].astype(F32).reshape(XR, wide[kind]).astype(BF16)
        own = w.at[rows_of(0), here]
        for j, d in enumerate(near_x):
            xcopies[g, kind, d] = put(own, own, xsem.at[g, i, j], at_x(d))

    def x_forward(g, kind):
        i = kinds.index(kind)
        for j, d in enumerate(near_x):
            xcopies[g, kind, d].wait_recv()
            if X == 4:
                half = w.at[rows_of(-d, 0 if d == 1 else HR, HR), wcols(g, c, kind, y)]
                xfcopies[g, kind, d] = put(half, half, xfsem.at[g, i, j], at_x(d))

    def x_last(g, kind):
        if X == 4:
            for d in near_x:
                xfcopies[g, kind, d].wait_recv()

    def y_start(g, d):
        blk = w.at[rows_of(d), wcols(g, c, "c", y)]
        for j, e in enumerate(near_y):
            ycopies[g, d, e] = put(blk, blk, ysem.at[g, d, j], at_y(e))

    def y_forward(g, d):
        for j, e in enumerate(near_y):
            ycopies[g, d, e].wait_recv()
            if Y == 4:
                half = w.at[rows_of(d, 0 if e == 1 else HR, HR), wcols(g, c, "c", yrel(-e))]
                yfcopies[g, d, e] = put(half, half, yfsem.at[g, d, j], at_y(e))

    def y_last(g):
        if Y == 4:
            for d in range(X):
                for e in near_y:
                    yfcopies[g, d, e].wait_recv()

    def hand_over(g, k, kind, yy=0):
        blk = w.at[:, wcols(g, c, kind, yy)]
        dcopies[g, k] = put(blk, blk, dsem.at[g, k], {"c": other})

    def hand_near(g):
        for e in near_y:
            hand_over(g, 1 + e, "c", yrel(e))

    def hand_last(g):
        y_last(g)
        if Y == 4:
            hand_over(g, 3, "c", yrel(2))

    def taken(g, keys):
        for k in keys:
            dcopies[g, k].wait_recv()

    def attend_a():
        taken(0, [0])
        lax.fori_loop(Y, HP, attend, 0)

    def attend_own():
        taken(0, [1])
        attend(y, 0)

    def attend_near():
        taken(0, [1 + e for e in near_y])
        lax.fori_loop(0, len(near_y), lambda i, carry: attend(lax.rem(y + 1 + i * (Y - 2), Y), carry), 0)

    def attend_far():
        if Y == 4:
            taken(0, [3])
            attend(yrel(2), 0)

    half_lane = iota((1, LANES), 1) < LANES // 2
    ones = [jnp.where(half_lane, 1.0, 0.0).astype(BF16), jnp.where(half_lane, 0.0, 1.0).astype(BF16)]

    def both(v):
        return jnp.concatenate([v * ones[0], v * ones[1]], axis=0)

    svec[...] = jnp.zeros_like(svec)

    def attend(h, carry):
        wqk = jnp.concatenate([w[:, cols(h * LANES, LANES)], w[:, cols(D + h * LANES, LANES)]], axis=1)
        qk[h] = dot(norm[...], wqk).astype(BF16)
        for p in range(NP):
            n_live = lens[p // CL, p % CL]
            live_key = iota((1, T), 1) < n_live
            live_row = iota((T, 1), 0) < n_live
            q2 = qk[h, p * T : (p + 1) * T, :LANES]
            k2 = qk[h, p * T : (p + 1) * T, LANES:]
            s = dot(both(q2), k2, 1, 1) + bias[pl.ds(2 * h, 2)].reshape(2 * T, T)
            s = jnp.where(live_key, s, NEG)
            e = jnp.exp(s - jnp.max(s, axis=1, keepdims=True))
            pr = (e * (1.0 / jnp.sum(e, axis=1, keepdims=True))).astype(BF16)
            prob[p, h] = pr
            for k in (0, 1):
                pk = jnp.where(live_row, pr[k * T : (k + 1) * T].astype(F32), 0.0)
                svec[p, pl.ds(2 * h + k, 1), :] = jnp.sum(pk, axis=0, keepdims=True)
        return carry

    z_start(0)
    z_start(1)
    x_start(0, "c")
    y_start(0, 0)
    x_start(0, "a")
    x_forward(0, "c")
    for d in near_x:
        y_start(0, d)
    x_start(1, "c")
    y_start(1, 0)
    y_forward(0, 0)
    x_forward(0, "a")
    x_start(1, "a")
    x_last(0, "c")
    if X == 4:
        y_start(0, 2)
    hand_over(0, 1, "c", y)
    for d in near_x:
        y_forward(0, d)
    x_last(0, "a")
    hand_over(0, 0, "a")
    x_forward(1, "c")
    for d in near_x:
        y_start(1, d)
    if X == 4:
        y_forward(0, 2)
    hand_near(0)
    x_forward(1, "a")
    y_forward(1, 0)
    loads[2].wait()
    attend_a()
    x_last(1, "c")
    if X == 4:
        y_start(1, 2)
    hand_last(0)
    hand_over(1, 1, "c", y)
    x_last(1, "a")
    hand_over(1, 0, "a")
    attend_own()
    for d in near_x:
        y_forward(1, d)
    attend_near()
    if X == 4:
        y_forward(1, 2)
    hand_near(1)
    attend_far()
    hand_last(1)
    for p in range(NP):
        avec[c, p * 16 : (p + 1) * 16, :] = dot(svec[p].astype(BF16), norm[p * T : (p + 1) * T, :]).astype(BF16)
    avec_copy = swap(avec.at[c], psem.at[1])
    taken(1, [0, 1] + [1 + e for e in near_y] + ([3] if Y == 4 else []))

    wv = w.at[:, 2 * D : 3 * D]
    wo = w.at[:, 3 * D : 4 * D]
    head_of = (iota((16, D), 1) // (D // H)) == iota((16, D), 0)
    prow = iota((NP, 1), 0)
    length, target = jnp.zeros((NP, 1), F32), jnp.zeros((NP, 1), F32)
    for p in range(NP):
        length = jnp.where(prow == p, lens[p // CL, p % CL].astype(F32), length)
        target = jnp.where(prow == p, labs[p // CL, p % CL].astype(F32), target)
    inv_len = 1.0 / length
    target = jnp.exp(target)

    zv = dot(avec[c], wv[...]).reshape(NP, 16, D)
    csum = jnp.sum(jnp.where(head_of[None], zv, 0.0), axis=1)
    pooled = hsum[...] * inv_len + dot((csum * inv_len).astype(BF16), wo[...])
    factor = lax.rsqrt(jnp.mean(pooled * pooled, axis=1, keepdims=True) + EPS)
    score = jnp.sum(pooled * factor * sw_row, axis=1, keepdims=True)

    exb[cand, 0] = jnp.broadcast_to(score, (NP, LANES))
    exb[cand, 1] = jnp.broadcast_to(target, (NP, LANES))
    ecopies = [put(exb.at[cand], exb.at[cand], esem.at[i], at_cand(i)) for i in range(1, Y * C)]
    for copy in ecopies:
        copy.wait_recv()
    scores, targets = exb[:, 0], exb[:, 1]
    query = iota((NP, LANES), 0) // CL

    def per_query(v, op, neutral):
        out = v
        for k in range(QL):
            out = jnp.where(query == k, op(jnp.where(query == k, v, neutral), axis=0, keepdims=True), out)
        return out

    highest = per_query(jnp.max(scores, axis=0), jnp.max, -jnp.inf)
    expsum = per_query(jnp.sum(jnp.exp(scores - highest[None]), axis=0), jnp.sum, 0.0)
    target_sum = per_query(jnp.sum(targets, axis=0), jnp.sum, 0.0)
    target_dot = per_query(jnp.sum(targets * scores, axis=0), jnp.sum, 0.0)
    losses = highest + jnp.log(expsum) - target_dot / target_sum
    for k in range(QL):
        loss[k] = jnp.max(losses[k * CL : k * CL + 1])
    sgrad = (jnp.exp(score - highest) / expsum - target / target_sum)[:, :1]

    along = jnp.sum(pooled * sw_row, axis=1, keepdims=True) * (1.0 / D)
    pooled_grad = sgrad * (factor * sw_row - pooled * (factor * factor * factor * along))
    g = (pooled_grad * inv_len).astype(BF16)
    cg = dot(g, wo[...], 1, 1)
    cexp = jnp.where(head_of[None], cg[:, None, :], 0.0).reshape(NP * 16, D).astype(BF16)
    tv = dot(cexp, wv[...], 1, 1).astype(BF16)
    for k, v in enumerate((csum.astype(BF16), g, cg.astype(BF16))):
        mixed[c, k] = v
    mixed_copy = swap(mixed.at[c], psem.at[2])
    for p in range(NP):
        uvec[p] = dot(tv[p * 16 : (p + 1) * 16], norm_t[c, :, p * T : (p + 1) * T])

    def keep(n, value):
        grad[:, :, n : n + value.shape[1]] = value.astype(BF16).reshape(X, XR, value.shape[1])

    def keep_outer():
        avec_copy.wait_recv()
        mixed_copy.wait_recv()
        mine = cols(c * DC, DC)
        sums = jnp.concatenate([mixed[k, 0].astype(F32) for k in range(C)], axis=0).astype(BF16)
        outs = jnp.concatenate([mixed[k, 1, :, mine].astype(F32) for k in range(C)], axis=0).astype(BF16)
        keep(0, dot(sums, outs, 0, 0))
        lane_head = (c * DC + iota((16, DC), 1)) // (D // H) == iota((16, DC), 0)
        total = 0.0
        for k in range(C):
            spread = jnp.where(lane_head[None], mixed[k, 2, :, mine].astype(F32)[:, None, :], 0.0).reshape(NP * 16, DC).astype(BF16)
            total += dot(avec[k], spread, 0, 0)
        keep(DC, total)

    a0c, b0c, a1c, b1c, a2c, b2c, z3c, obc = {}, {}, {}, {}, {}, {}, {}, {}

    def lanes_of(t, yy=None):
        return pl.ds(t * NC, NC) if yy is None else cols(t * NC + yy * NB, NB)

    def reduce_1(t):
        if X == 4:
            far = lax.rem(x + 2, X)
            for j, d in enumerate(near_x):
                half = grad.at[far, j * HQ : (j + 1) * HQ, lanes_of(t)]
                a0c[t, j] = put(half, a0.at[t, j], a0sem.at[t, j], at_x(d))
        if Y == 4:
            for j, e in enumerate(near_y):
                half = grad.at[:, HR + j * HQ : HR + (j + 1) * HQ, lanes_of(t, yrel(2))]
                b0c[t, j] = put(half, b0.at[t, j], b0sem.at[t, j], at_y(e))

    def reduce_1b(t):
        for j, d in enumerate(near_x):
            ahead = lax.rem(x + d, X)
            if X == 4:
                a0c[t, j].wait_recv()
                part = pl.ds(j * HQ, HQ)
                grad[ahead, part, lanes_of(t)] = (grad[ahead, part, lanes_of(t)].astype(F32) + a0[t, j].astype(F32)).astype(BF16)
            a1c[t, j] = put(grad.at[ahead, :HR, lanes_of(t)], a1.at[t, j], a1sem.at[t, j], at_x(d))
        for j, e in enumerate(near_y):
            ahead = lanes_of(t, yrel(e))
            if Y == 4:
                b0c[t, j].wait_recv()
                part = pl.ds(HR + j * HQ, HQ)
                grad[:, part, ahead] = (grad[:, part, ahead].astype(F32) + b0[t, j].astype(F32)).astype(BF16)
            b1c[t, j] = put(grad.at[:, HR:, ahead], b1.at[t, j], b1sem.at[t, j], at_y(e))

    def reduce_2(t):
        total = grad[x, :HR, lanes_of(t)].astype(F32)
        for j in range(len(near_x)):
            a1c[t, j].wait_recv()
            total += a1[t, j].astype(F32)
        a1s[t] = total.astype(BF16)
        total = grad[:, HR:, lanes_of(t, y)].astype(F32)
        for j in range(len(near_y)):
            b1c[t, j].wait_recv()
            total += b1[t, j].astype(F32)
        b1s[t] = total.astype(BF16)
        for d in range(1, Y):
            a2c[t, d] = put(a1s.at[t, :, cols(lax.rem(y + d, Y) * NB, NB)], a2.at[t, d - 1], a2sem.at[t, d], at_y(d))
        for d in range(1, X):
            b2c[t, d] = put(b1s.at[t, lax.rem(x + d, X)], b2.at[t, d - 1], b2sem.at[t, d], at_x(d))

    def reduce_3(t):
        total = a1s[t, :, cols(y * NB, NB)].astype(F32)
        for d in range(1, Y):
            a2c[t, d].wait_recv()
            total += a2[t, d - 1].astype(F32)
        zs[t, :ZH] = total.reshape(ZH, R, NB).astype(BF16)
        total = b1s[t, x].astype(F32)
        for d in range(1, X):
            b2c[t, d].wait_recv()
            total += b2[t, d - 1].astype(F32)
        zs[t, ZH:] = total.reshape(ZH, R, NB).astype(BF16)
        for d in range(1, Z):
            z3c[t, d] = put(zs.at[t, lax.rem(z + d, Z)], z3.at[t, d - 1], z3sem.at[t, d], at_z(d))

    def reduce_4(t):
        total = zs[t, z].astype(F32)
        for d in range(1, Z):
            z3c[t, d].wait_recv()
            total += z3[t, d - 1].astype(F32)
        ob[t, cand] = total.astype(BF16)
        for i in range(1, Y * C):
            obc[t, i] = put(ob.at[t, cand], ob.at[t, cand], obsem.at[t, i], at_cand(i))

    def backward(h, out):
        for p in range(NP):
            n_live = lens[p // CL, p % CL]
            live_row = iota((T, 1), 0) < n_live
            rows = pl.ds(p * T, T)
            pr = prob[p, h].astype(F32).reshape(2, T, T)
            ds = []
            for k in (0, 1):
                pu = pr[k] * uvec[p, pl.ds(2 * h + k, 1), :]
                mean = jnp.sum(pu, axis=1, keepdims=True)
                ds.append(jnp.where(live_row, pu - pr[k] * mean, 0.0).astype(BF16))
            out[rows, :LANES] = dot(jnp.concatenate(ds, axis=1), both(qk[h, rows, LANES:])).astype(BF16)
            out[rows, LANES:] = dot(jnp.concatenate(ds, axis=0), both(qk[h, rows, :LANES]), 0, 0).astype(BF16)

    def dqk_copy(i):
        return pltpu.make_async_remote_copy(
            dsend.at[i], dqk.at[i, c], qsem.at[0, i], qsem.at[1, i], device_id={"c": other}, device_id_type=MESH
        )

    def for_partner(i, carry):
        backward(other * HC + i, dsend.at[i])
        dqk_copy(i).start()
        return carry

    def for_self(i, carry):
        backward(c * HC + i, dqk.at[i, c])
        dqk_copy(i).wait()
        dw = dot(norm_t[0], dqk[i, 0]) + dot(norm_t[1], dqk[i, 1])
        grad[:, :, cols(2 * DC + i * 2 * LANES, 2 * LANES)] = dw.astype(BF16).reshape(X, XR, 2 * LANES)
        return carry

    lax.fori_loop(0, HC, for_partner, 0)
    keep_outer()
    norm_copy.wait_recv()
    reduce_1(0)
    lax.fori_loop(0, 1, for_self, 0)
    reduce_1(1)
    reduce_1b(0)
    lax.fori_loop(1, HC, for_self, 0)
    reduce_1(2)
    reduce_2(0)
    reduce_1b(1)
    reduce_1b(2)
    reduce_3(0)
    reduce_2(1)
    reduce_2(2)
    reduce_3(1)
    reduce_4(0)
    reduce_3(2)
    reduce_4(1)
    reduce_4(2)
    squares = jnp.zeros((R, NB), F32)
    for t in range(PARTS):
        v = ob[t, cand].astype(F32)
        squares += v * v
    squares = jnp.sum(jnp.sum(squares, axis=1, keepdims=True), axis=0, keepdims=True)
    sqz[z] = jnp.broadcast_to(squares, (8, LANES))
    zsq = [put(sqz.at[z], sqz.at[z], sqzsem.at[d], at_z(d)) for d in range(1, Z)]
    for copy in obc.values():
        copy.wait_recv()
    for t in range(PARTS):
        for k in range(Y * C):
            for m in range(NB // LANES):
                b, core = (t * NC + (k // C) * NB) // LANES + m, k % C
                outer = DC // LANES
                if b < outer:
                    n = 3 * D + core * DC + b * LANES
                elif b < 2 * outer:
                    n = 2 * D + core * DC + (b - outer) * LANES
                else:
                    n = (b - 2 * outer) % 2 * D + (core * HC + (b - 2 * outer) // 2) * LANES
                upd[:, n : n + LANES] = ob[t, k, :, m * LANES : (m + 1) * LANES]
    for copy in zsq:
        copy.wait_recv()
    me = x * Y * C + cand
    sq[me] = jnp.sum(sqz[...], axis=0)

    def sq_copy(i):
        to = at_cand(lax.rem(i, Y * C)) | at_x(i // (Y * C))
        return pltpu.make_async_remote_copy(sq.at[me], sq.at[me], sqsem.at[0, i], sqsem.at[1, i], device_id=to, device_id_type=MESH)

    def sq_start(i, carry):
        sq_copy(i).start()
        return carry

    def sq_wait(i, carry):
        sq_copy(i).wait()
        return carry

    lax.fori_loop(1, X * Y * C, sq_start, 0)
    lax.fori_loop(1, X * Y * C, sq_wait, 0)
    total_out[0] = jnp.max(jnp.sum(sq[...], axis=0))
    for copy in started:
        copy.wait_send()


def solution(mesh):
    n_dp, n_cand = mesh.shape["dp"], mesh.shape["cand"]
    X, C = (4 if n_dp == 32 else 2), 2
    Z, Y = n_dp // X, n_cand // C
    split = Mesh(mesh.devices.reshape(X, Z, Y, C), ("x", "z", "y", "c"))
    dp, cand = ("x", "z"), ("y", "c")

    def shards(hidden, attn_weight, norm_gain, pos_bias, score_weight, pair_lengths, labels):
        QL, CL, T, D = hidden.shape
        H = pos_bias.shape[0]
        R = attn_weight.shape[0]
        NP, XR, NC = QL * CL, Z * R, 4 * D // PARTS // C
        HR, NB = XR // 2, NC // Y
        hbm = pl.BlockSpec(memory_space=pl.ANY)
        vmem, smem = pl.BlockSpec(memory_space=pltpu.VMEM), pl.BlockSpec(memory_space=pltpu.SMEM)
        dma = pltpu.SemaphoreType.DMA
        V = pltpu.VMEM
        summed, loss, squares = pl.pallas_call(
            functools.partial(step_kernel, (X, Z, Y, C)),
            out_shape=(
                jax.ShapeDtypeStruct((R, 4 * D), BF16),
                jax.ShapeDtypeStruct((QL,), F32),
                jax.ShapeDtypeStruct((1,), F32),
            ),
            in_specs=[hbm, hbm, vmem, hbm, vmem, smem, smem],
            out_specs=(vmem, smem, smem),
            scratch_shapes=[
                V(hidden.shape, BF16),
                V(attn_weight.shape, BF16),
                V(pos_bias.shape, F32),
                V((NP * T, D), BF16),
                V((C, D, NP * T), BF16),
                V((D, 4 * D), BF16),
                V((H // 2, NP * T, 2 * LANES), BF16),
                V((NP, H // 2, 2 * T, T), BF16),
                V((X, XR, 4 * D // C), BF16),
                V((NP, D), F32),
                V((NP, 16, T), F32),
                V((C, NP * 16, D), BF16),
                V((NP, 16, T), F32),
                V((H // 2 // C, C, NP * T, 2 * LANES), BF16),
                V((H // 2 // C, NP * T, 2 * LANES), BF16),
                V((C, 3, NP, D), BF16),
                V((2, Z, R, LANES), BF16),
                V((2, Z, R, D - Y * LANES), BF16),
                V((Y * C, 2, NP, LANES), F32),
                V((PARTS, 2, HR // 2, NC), BF16),
                V((PARTS, 2, X, HR // 2, NB), BF16),
                V((PARTS, 2, HR, NC), BF16),
                V((PARTS, HR, NC), BF16),
                V((PARTS, 2, X, HR, NB), BF16),
                V((PARTS, X, HR, NB), BF16),
                V((PARTS, Y - 1, HR, NB), BF16),
                V((PARTS, X - 1, HR, NB), BF16),
                V((PARTS, Z, R, NB), BF16),
                V((PARTS, Z - 1, R, NB), BF16),
                V((PARTS, Y * C, R, NB), BF16),
                V((Z, 8, LANES), F32),
                V((X * Y * C, 8, LANES), F32),
                dma((3,)),
                dma((2, 2, Z, 2)),
                dma((2, 2, 2, 2)),
                dma((2, 2, 2, 2)),
                dma((2, X, 2, 2)),
                dma((2, X, 2, 2)),
                dma((2, 1 + Y, 2)),
                dma((3, 2)),
                dma((2, H // 2 // C)),
                dma((Y * C, 2)),
                dma((PARTS, 2, 2)),
                dma((PARTS, 2, 2)),
                dma((PARTS, 2, 2)),
                dma((PARTS, 2, 2)),
                dma((PARTS, Y, 2)),
                dma((PARTS, X, 2)),
                dma((PARTS, Z, 2)),
                dma((PARTS, Y * C, 2)),
                dma((Z, 2)),
                dma((2, X * Y * C)),
            ],
            compiler_params=pltpu.CompilerParams(collective_id=0, has_side_effects=True, vmem_limit_bytes=60 * 2**20),
        )(hidden, attn_weight, norm_gain, pos_bias, score_weight, pair_lengths, labels)
        scale = 1.0 / (jnp.sqrt(squares[0] / (4.0 * D * D)) + EPS)
        return summed.astype(F32) * scale, loss

    placed = (P(dp, cand, None, None), P(dp, None), P(), P(), P(), P(dp, cand), P(dp, cand))
    return jax.shard_map(shards, mesh=split, in_specs=placed, out_specs=(P(dp, None), P(dp)), check_vma=False)
```

```python
import functools

import jax
import jax.numpy as jnp
from jax import lax
from jax.experimental import pallas as pl
from jax.experimental.pallas import tpu as pltpu
from jax.sharding import Mesh
from jax.sharding import PartitionSpec as P

EPS = 1e-06
MESH = pl.DeviceIdType.MESH
F32, BF16 = jnp.float32, jnp.bfloat16
NEG = -1e30
PARTS = 3
LANES = 128


def dot(a, b, ca=1, cb=0):
    return lax.dot_general(a, b, (((ca,), (cb,)), ((), ())), preferred_element_type=F32)


def iota(shape, axis):
    return lax.broadcasted_iota(jnp.int32, shape, axis)


def step_kernel(dims, hid_in, wsh_in, gain, bias_in, sw, lens, labs, upd, out_s, hid, wsh, bias, norm, norm_t, w, qk, prob, grad,
                hsum, svec, avec, uvec, dqk, dsend, mixed, zc, za, zv, exb, a0, b0, a1, a1s, b1, b1s, a2, b2, zs, z3, ob, sqz, sq,
                lsem, zsem, xsem, xfsem, ysem, yfsem, dsem, psem, qsem, esem, a0sem, b0sem, a1sem, b1sem, a2sem, b2sem, z3sem, obsem,
                sqzsem, sqsem):
    X, Z, Y, C = dims
    QL, CL, T, D = hid.shape
    H = bias.shape[0]
    HP = H // 2
    HC = HP // C
    DC = D // C
    NP = QL * CL
    R = wsh.shape[0]
    XR = Z * R
    HR = XR // 2
    HQ = HR // 2
    ZH = Z // 2
    NC = 4 * D // PARTS // C
    NB = NC // Y
    x, z, y, c = (lax.axis_index(name) for name in ("x", "z", "y", "c"))
    other = 1 - c
    cand = y * C + c
    started = []

    def at_x(d):
        return {"x": lax.rem(x + d, X)}

    def at_z(d):
        return {"z": lax.rem(z + d, Z)}

    def at_y(d):
        return {"y": lax.rem(y + d, Y)}

    def at_cand(i):
        return {"y": lax.rem(y + i // C, Y), "c": lax.rem(c + i % C, C)}

    def put(src, dst, sems, to):
        copy = pltpu.make_async_remote_copy(src, dst, sems.at[0], sems.at[1], device_id=to, device_id_type=MESH)
        copy.start()
        started.append(copy)
        return copy

    def cols(n, width):
        return pl.ds(pl.multiple_of(n, LANES), width)

    loads = [pltpu.make_async_copy(src, dst, lsem.at[i]) for i, (src, dst) in enumerate(((hid_in, hid), (wsh_in, wsh), (bias_in, bias)))]
    for load in loads:
        load.start()

    near_x = [1] if X == 2 else [1, X - 1]
    near_y = [1] if Y == 2 else [1, Y - 1]
    first = [at_z(d) for d in range(1, Z)] + [at_x(d) for d in near_x] + [at_y(d) for d in near_y] + [{"c": other}]
    bar = pltpu.get_barrier_semaphore()
    for to in first:
        pl.semaphore_signal(bar, 1, device_id=to, device_id_type=MESH)

    def pair_len(p):
        return lens[p // CL, lax.rem(p, CL)]

    def normalise(p, carry):
        v = hid[p // CL, lax.rem(p, CL)].astype(F32)
        n = v * lax.rsqrt(jnp.mean(v * v, axis=1, keepdims=True) + EPS) * gain_row
        rows = pl.ds(pl.multiple_of(p * T, T), T)
        norm[rows, :] = n.astype(BF16)
        norm_t[c, :, cols(p * T, T)] = n.T.astype(BF16)
        live = iota((T, 1), 0) < pair_len(p)
        hsum[pl.ds(p, 1), :] = jnp.sum(jnp.where(live, v, 0.0), axis=0, keepdims=True)
        return carry

    gain_row, sw_row = gain[...].reshape(1, D), sw[...].reshape(1, D)
    loads[1].wait()
    pl.semaphore_wait(bar, len(first))

    def swap(ref, sem):
        return put(ref, ref, sem, {"c": other})


    AW = D - Y * LANES
    wide = {"c": LANES, "a": AW, 0: 2 * LANES, 1: 2 * LANES, 2: 2 * LANES}
    kinds = {0: ("c", "a"), 1: (0, 1, 2)}

    def wcols(g, core, kind, yy=0):
        base = (2 * g + core) * D
        return cols(base + (yy * LANES if kind == "c" else Y * LANES if kind == "a" else kind * 2 * LANES), wide[kind])

    def yrel(e):
        return lax.rem(y + e + Y, Y)

    def rows_of(d, lo=0, n=XR):
        return pl.ds(pl.multiple_of(lax.rem(x + d + X, X) * XR + lo, HR), n)

    zcopies, xcopies, xfcopies, ycopies, yfcopies, dcopies = {}, {}, {}, {}, {}, {}
    zbuf = {"c": zc, "a": za, 0: zv.at[0], 1: zv.at[1], 2: zv.at[2]}

    def z_start(g):
        for i, kind in enumerate(kinds[g]):
            here = wcols(g, c, kind, y)
            for d in range(1, Z):
                zcopies[g, kind, d] = put(wsh.at[:, here], zbuf[kind].at[z], zsem.at[g, i, d], at_z(d))
            zbuf[kind][z] = wsh[:, here]

    def x_start(g, kind):
        i = kinds[g].index(kind)
        for d in range(1, Z):
            zcopies[g, kind, d].wait_recv()
        here = wcols(g, c, kind, y)
        w[rows_of(0), here] = zbuf[kind][...].astype(F32).reshape(XR, wide[kind]).astype(BF16)
        own = w.at[rows_of(0), here]
        for j, d in enumerate(near_x):
            xcopies[g, kind, d] = put(own, own, xsem.at[g, i, j], at_x(d))

    def x_forward(g, kind):
        i = kinds[g].index(kind)
        for j, d in enumerate(near_x):
            xcopies[g, kind, d].wait_recv()
            if X == 4:
                half = w.at[rows_of(-d, 0 if d == 1 else HR, HR), wcols(g, c, kind, y)]
                xfcopies[g, kind, d] = put(half, half, xfsem.at[g, i, j], at_x(d))

    def x_last(g, kind):
        if X == 4:
            for d in near_x:
                xfcopies[g, kind, d].wait_recv()

    def y_start(g, d):
        blk = w.at[rows_of(d), wcols(g, c, "c", y)]
        for j, e in enumerate(near_y):
            ycopies[g, d, e] = put(blk, blk, ysem.at[g, d, j], at_y(e))

    def y_forward(g, d):
        for j, e in enumerate(near_y):
            ycopies[g, d, e].wait_recv()
            if Y == 4:
                half = w.at[rows_of(d, 0 if e == 1 else HR, HR), wcols(g, c, "c", yrel(-e))]
                yfcopies[g, d, e] = put(half, half, yfsem.at[g, d, j], at_y(e))

    def y_last(g):
        if Y == 4:
            for d in range(X):
                for e in near_y:
                    yfcopies[g, d, e].wait_recv()

    def hand_over(g, k, kind, yy=0):
        blk = w.at[:, wcols(g, c, kind, yy)]
        dcopies[g, k] = put(blk, blk, dsem.at[g, k], {"c": other})

    def hand_near(g):
        for e in near_y:
            hand_over(g, 1 + e, "c", yrel(e))

    def hand_last(g):
        y_last(g)
        if Y == 4:
            hand_over(g, 3, "c", yrel(2))

    def taken(g, keys):
        for k in keys:
            dcopies[g, k].wait_recv()

    def attend_a():
        taken(0, [0])
        lax.fori_loop(Y, HP, attend, 0)

    def attend_own():
        taken(0, [1])
        attend(y, 0)

    def attend_near():
        taken(0, [1 + e for e in near_y])
        lax.fori_loop(0, len(near_y), lambda i, carry: attend(lax.rem(y + 1 + i * (Y - 2), Y), carry), 0)

    def attend_far():
        if Y == 4:
            taken(0, [3])
            attend(yrel(2), 0)

    half_lane = iota((1, LANES), 1) < LANES // 2
    ones = [jnp.where(half_lane, 1.0, 0.0).astype(BF16), jnp.where(half_lane, 0.0, 1.0).astype(BF16)]

    def both(v):
        return jnp.concatenate([v * ones[0], v * ones[1]], axis=0)

    svec[...] = jnp.zeros_like(svec)

    def attend(h, carry):
        wqk = jnp.concatenate([w[:, cols(h * LANES, LANES)], w[:, cols(D + h * LANES, LANES)]], axis=1)
        qk[h] = dot(norm[...], wqk).astype(BF16)
        for p in range(NP):
            n_live = lens[p // CL, p % CL]
            live_key = iota((1, T), 1) < n_live
            live_row = iota((T, 1), 0) < n_live
            q2 = qk[h, p * T : (p + 1) * T, :LANES]
            k2 = qk[h, p * T : (p + 1) * T, LANES:]
            s = dot(both(q2), k2, 1, 1) + bias[pl.ds(2 * h, 2)].reshape(2 * T, T)
            s = jnp.where(live_key, s, NEG)
            e = jnp.exp(s - jnp.max(s, axis=1, keepdims=True))
            pr = (e * (1.0 / jnp.sum(e, axis=1, keepdims=True))).astype(BF16)
            prob[p, h] = pr
            for k in (0, 1):
                pk = jnp.where(live_row, pr[k * T : (k + 1) * T].astype(F32), 0.0)
                svec[p, pl.ds(2 * h + k, 1), :] = jnp.sum(pk, axis=0, keepdims=True)
        return carry

    z_start(0)
    z_start(1)
    loads[0].wait()
    lax.fori_loop(0, NP, normalise, 0)
    norm_copy = swap(norm_t.at[c], psem.at[0])
    x_start(0, "c")
    y_start(0, 0)
    x_start(0, "a")
    x_forward(0, "c")
    for d in near_x:
        y_start(0, d)
    y_forward(0, 0)
    x_forward(0, "a")
    x_start(1, 0)
    x_last(0, "c")
    if X == 4:
        y_start(0, 2)
    hand_over(0, 1, "c", y)
    for d in near_x:
        y_forward(0, d)
    x_last(0, "a")
    hand_over(0, 0, "a")
    x_start(1, 1)
    x_start(1, 2)
    if X == 4:
        y_forward(0, 2)
    hand_near(0)
    loads[2].wait()
    attend_a()
    x_forward(1, 0)
    x_forward(1, 1)
    attend_own()
    hand_last(0)
    x_forward(1, 2)
    attend_near()
    for k in kinds[1]:
        x_last(1, k)
        hand_over(1, k, k)
    attend_far()
    for p in range(NP):
        avec[c, p * 16 : (p + 1) * 16, :] = dot(svec[p].astype(BF16), norm[p * T : (p + 1) * T, :]).astype(BF16)
    avec_copy = swap(avec.at[c], psem.at[1])
    taken(1, kinds[1])

    wv = w.at[:, 2 * D : 3 * D]
    wo = w.at[:, 3 * D : 4 * D]
    head_of = (iota((16, D), 1) // (D // H)) == iota((16, D), 0)
    prow = iota((NP, 1), 0)
    length, target = jnp.zeros((NP, 1), F32), jnp.zeros((NP, 1), F32)
    for p in range(NP):
        length = jnp.where(prow == p, lens[p // CL, p % CL].astype(F32), length)
        target = jnp.where(prow == p, labs[p // CL, p % CL].astype(F32), target)
    inv_len = 1.0 / length
    target = jnp.exp(target)

    zv = dot(avec[c], wv[...]).reshape(NP, 16, D)
    csum = jnp.sum(jnp.where(head_of[None], zv, 0.0), axis=1)
    pooled = hsum[...] * inv_len + dot((csum * inv_len).astype(BF16), wo[...])
    factor = lax.rsqrt(jnp.mean(pooled * pooled, axis=1, keepdims=True) + EPS)
    score = jnp.sum(pooled * factor * sw_row, axis=1, keepdims=True)

    exb[cand, 0] = jnp.broadcast_to(score, (NP, LANES))
    exb[cand, 1] = jnp.broadcast_to(target, (NP, LANES))
    ecopies = [put(exb.at[cand], exb.at[cand], esem.at[i], at_cand(i)) for i in range(1, Y * C)]

    along = jnp.sum(pooled * sw_row, axis=1, keepdims=True) * (1.0 / D)
    unit = (factor * sw_row - pooled * (factor * factor * factor * along)) * inv_len
    unit_b = unit.astype(BF16)
    cg = dot(unit_b, wo[...], 1, 1)
    for k, v in enumerate((csum.astype(BF16), unit_b, cg.astype(BF16))):
        mixed[c, k] = v
    mixed_copy = swap(mixed.at[c], psem.at[2])
    cexp = jnp.where(head_of[None], cg[:, None, :], 0.0).reshape(NP * 16, D).astype(BF16)
    tv = dot(cexp, wv[...], 1, 1).astype(BF16)
    for p in range(NP):
        uvec[p] = dot(tv[p * 16 : (p + 1) * 16], norm_t[c, :, p * T : (p + 1) * T])

    def listwise():
        for copy in ecopies:
            copy.wait_recv()
        scores, targets = exb[:, 0], exb[:, 1]
        query = iota((NP, LANES), 0) // CL

        def per_query(v, op, neutral):
            out = v
            for k in range(QL):
                out = jnp.where(query == k, op(jnp.where(query == k, v, neutral), axis=0, keepdims=True), out)
            return out

        highest = per_query(jnp.max(scores, axis=0), jnp.max, -jnp.inf)
        expsum = per_query(jnp.sum(jnp.exp(scores - highest[None]), axis=0), jnp.sum, 0.0)
        target_sum = per_query(jnp.sum(targets, axis=0), jnp.sum, 0.0)
        target_dot = per_query(jnp.sum(targets * scores, axis=0), jnp.sum, 0.0)
        losses = highest + jnp.log(expsum) - target_dot / target_sum
        for k in range(QL):
            out_s[1 + k] = jnp.max(losses[k * CL : k * CL + 1])
        grads = []
        for k in range(C):
            grads.append((jnp.exp(exb[y * C + k, 0] - highest) / expsum - exb[y * C + k, 1] / target_sum)[:, :1])
        return grads

    def keep(n, value):
        grad[:, :, n : n + value.shape[1]] = value.astype(BF16).reshape(X, XR, value.shape[1])

    def keep_outer(sgrad):
        avec_copy.wait_recv()
        mixed_copy.wait_recv()
        mine = cols(c * DC, DC)
        sums = jnp.concatenate([mixed[k, 0].astype(F32) for k in range(C)], axis=0).astype(BF16)
        outs = jnp.concatenate([mixed[k, 1, :, mine].astype(F32) * sgrad[k] for k in range(C)], axis=0).astype(BF16)
        keep(0, dot(sums, outs, 0, 0))
        lane_head = (c * DC + iota((16, DC), 1)) // (D // H) == iota((16, DC), 0)
        total = 0.0
        for k in range(C):
            rows = mixed[k, 2, :, mine].astype(F32) * sgrad[k]
            spread = jnp.where(lane_head[None], rows[:, None, :], 0.0).reshape(NP * 16, DC).astype(BF16)
            total += dot(avec[k], spread, 0, 0)
        keep(DC, total)

    def scale_norm(sgrad):
        norm_copy.wait_recv()
        norm_copy.wait_send()
        for k in range(C):
            for p in range(NP):
                v = norm_t[k, :, p * T : (p + 1) * T].astype(F32) * sgrad[k][p : p + 1]
                norm_t[k, :, p * T : (p + 1) * T] = v.astype(BF16)

    a0c, b0c, a1c, b1c, a2c, b2c, z3c, obc = {}, {}, {}, {}, {}, {}, {}, {}

    def lanes_of(t, yy=None):
        return pl.ds(t * NC, NC) if yy is None else cols(t * NC + yy * NB, NB)

    def reduce_1(t):
        if X == 4:
            far = lax.rem(x + 2, X)
            for j, d in enumerate(near_x):
                half = grad.at[far, j * HQ : (j + 1) * HQ, lanes_of(t)]
                a0c[t, j] = put(half, a0.at[t, j], a0sem.at[t, j], at_x(d))
        if Y == 4:
            for j, e in enumerate(near_y):
                half = grad.at[:, HR + j * HQ : HR + (j + 1) * HQ, lanes_of(t, yrel(2))]
                b0c[t, j] = put(half, b0.at[t, j], b0sem.at[t, j], at_y(e))

    def reduce_1b(t):
        for j, d in enumerate(near_x):
            ahead = lax.rem(x + d, X)
            if X == 4:
                a0c[t, j].wait_recv()
                part = pl.ds(j * HQ, HQ)
                grad[ahead, part, lanes_of(t)] = (grad[ahead, part, lanes_of(t)].astype(F32) + a0[t, j].astype(F32)).astype(BF16)
            a1c[t, j] = put(grad.at[ahead, :HR, lanes_of(t)], a1.at[t, j], a1sem.at[t, j], at_x(d))
        for j, e in enumerate(near_y):
            ahead = lanes_of(t, yrel(e))
            if Y == 4:
                b0c[t, j].wait_recv()
                part = pl.ds(HR + j * HQ, HQ)
                grad[:, part, ahead] = (grad[:, part, ahead].astype(F32) + b0[t, j].astype(F32)).astype(BF16)
            b1c[t, j] = put(grad.at[:, HR:, ahead], b1.at[t, j], b1sem.at[t, j], at_y(e))

    def reduce_2(t):
        total = grad[x, :HR, lanes_of(t)].astype(F32)
        for j in range(len(near_x)):
            a1c[t, j].wait_recv()
            total += a1[t, j].astype(F32)
        a1s[t] = total.astype(BF16)
        total = grad[:, HR:, lanes_of(t, y)].astype(F32)
        for j in range(len(near_y)):
            b1c[t, j].wait_recv()
            total += b1[t, j].astype(F32)
        b1s[t] = total.astype(BF16)
        for d in range(1, Y):
            a2c[t, d] = put(a1s.at[t, :, cols(lax.rem(y + d, Y) * NB, NB)], a2.at[t, d - 1], a2sem.at[t, d], at_y(d))
        for d in range(1, X):
            b2c[t, d] = put(b1s.at[t, lax.rem(x + d, X)], b2.at[t, d - 1], b2sem.at[t, d], at_x(d))

    def reduce_3(t):
        total = a1s[t, :, cols(y * NB, NB)].astype(F32)
        for d in range(1, Y):
            a2c[t, d].wait_recv()
            total += a2[t, d - 1].astype(F32)
        zs[t, :ZH] = total.reshape(ZH, R, NB).astype(BF16)
        total = b1s[t, x].astype(F32)
        for d in range(1, X):
            b2c[t, d].wait_recv()
            total += b2[t, d - 1].astype(F32)
        zs[t, ZH:] = total.reshape(ZH, R, NB).astype(BF16)
        for d in range(1, Z):
            z3c[t, d] = put(zs.at[t, lax.rem(z + d, Z)], z3.at[t, d - 1], z3sem.at[t, d], at_z(d))

    def reduce_4(t):
        total = zs[t, z].astype(F32)
        for d in range(1, Z):
            z3c[t, d].wait_recv()
            total += z3[t, d - 1].astype(F32)
        ob[t, cand] = total.astype(BF16)
        for i in range(1, Y * C):
            obc[t, i] = put(ob.at[t, cand], ob.at[t, cand], obsem.at[t, i], at_cand(i))

    def backward(h, out):
        for p in range(NP):
            n_live = lens[p // CL, p % CL]
            live_row = iota((T, 1), 0) < n_live
            rows = pl.ds(p * T, T)
            pr = prob[p, h].astype(F32).reshape(2, T, T)
            ds = []
            for k in (0, 1):
                pu = pr[k] * uvec[p, pl.ds(2 * h + k, 1), :]
                mean = jnp.sum(pu, axis=1, keepdims=True)
                ds.append(jnp.where(live_row, pu - pr[k] * mean, 0.0).astype(BF16))
            out[rows, :LANES] = dot(jnp.concatenate(ds, axis=1), both(qk[h, rows, LANES:])).astype(BF16)
            out[rows, LANES:] = dot(jnp.concatenate(ds, axis=0), both(qk[h, rows, :LANES]), 0, 0).astype(BF16)

    def dqk_copy(i):
        return pltpu.make_async_remote_copy(
            dsend.at[i], dqk.at[i, c], qsem.at[0, i], qsem.at[1, i], device_id={"c": other}, device_id_type=MESH
        )

    def for_partner(i, carry):
        backward(other * HC + i, dsend.at[i])
        dqk_copy(i).start()
        return carry

    def for_self(i, carry):
        backward(c * HC + i, dqk.at[i, c])
        return carry

    def keep_qk(i, carry):
        dqk_copy(i).wait()
        dw = dot(norm_t[0], dqk[i, 0]) + dot(norm_t[1], dqk[i, 1])
        grad[:, :, cols(2 * DC + i * 2 * LANES, 2 * LANES)] = dw.astype(BF16).reshape(X, XR, 2 * LANES)
        return carry

    lax.fori_loop(0, HC, for_partner, 0)
    lax.fori_loop(0, HC, for_self, 0)
    sgrad = listwise()
    keep_outer(sgrad)
    reduce_1(0)
    scale_norm(sgrad)
    keep_qk(0, 0)
    reduce_1(1)
    lax.fori_loop(1, HC, keep_qk, 0)
    reduce_1(2)
    reduce_1b(0)
    reduce_1b(1)
    reduce_1b(2)
    reduce_2(0)
    reduce_2(1)
    reduce_2(2)
    reduce_3(0)
    reduce_3(1)
    reduce_3(2)
    reduce_4(0)
    reduce_4(1)
    reduce_4(2)
    squares = jnp.zeros((R, NB), F32)
    for t in range(PARTS):
        v = ob[t, cand].astype(F32)
        squares += v * v
    squares = jnp.sum(jnp.sum(squares, axis=1, keepdims=True), axis=0, keepdims=True)
    sqz[z] = jnp.broadcast_to(squares, (8, LANES))
    zline = sqz.at[z, :1]
    zsq = [put(zline, zline, sqzsem.at[d], at_z(d)) for d in range(1, Z)]
    for copy in obc.values():
        copy.wait_recv()
    for t in range(PARTS):
        for k in range(Y * C):
            for m in range(NB // LANES):
                b, core = (t * NC + (k // C) * NB) // LANES + m, k % C
                outer = DC // LANES
                if b < outer:
                    n = 3 * D + core * DC + b * LANES
                elif b < 2 * outer:
                    n = 2 * D + core * DC + (b - outer) * LANES
                else:
                    n = (b - 2 * outer) % 2 * D + (core * HC + (b - 2 * outer) // 2) * LANES
                upd[:, n : n + LANES] = ob[t, k, :, m * LANES : (m + 1) * LANES]
    for copy in zsq:
        copy.wait_recv()
    me = x * Y * C + cand
    sq[me, :1] = jnp.sum(sqz[:, :1], axis=0)
    line = sq.at[me, :1]
    sqs = [put(line, line, sqsem.at[i], at_cand(i % (Y * C)) | at_x(i // (Y * C))) for i in range(1, X * Y * C)]
    for copy in sqs:
        copy.wait_recv()
    out_s[0] = jnp.max(jnp.sum(sq[:, :1], axis=0))
    for copy in started:
        if copy is not norm_copy:
            copy.wait_send()


def solution(mesh):
    n_dp, n_cand = mesh.shape["dp"], mesh.shape["cand"]
    X, C = (4 if n_dp == 32 else 2), 2
    Z, Y = n_dp // X, n_cand // C
    split = Mesh(mesh.devices.reshape(X, Z, Y, C), ("x", "z", "y", "c"))
    dp, cand = ("x", "z"), ("y", "c")

    def shards(hidden, attn_weight, norm_gain, pos_bias, score_weight, pair_lengths, labels):
        QL, CL, T, D = hidden.shape
        H = pos_bias.shape[0]
        R = attn_weight.shape[0]
        NP, XR, NC = QL * CL, Z * R, 4 * D // PARTS // C
        HR, NB = XR // 2, NC // Y
        hbm = pl.BlockSpec(memory_space=pl.ANY)
        vmem, smem = pl.BlockSpec(memory_space=pltpu.VMEM), pl.BlockSpec(memory_space=pltpu.SMEM)
        dma = pltpu.SemaphoreType.DMA
        V = pltpu.VMEM
        summed, scalars = pl.pallas_call(
            functools.partial(step_kernel, (X, Z, Y, C)),
            out_shape=(
                jax.ShapeDtypeStruct((R, 4 * D), BF16),
                jax.ShapeDtypeStruct((1 + QL,), F32),
            ),
            in_specs=[hbm, hbm, vmem, hbm, vmem, smem, smem],
            out_specs=(vmem, smem),
            scratch_shapes=[
                V(hidden.shape, BF16),
                V(attn_weight.shape, BF16),
                V(pos_bias.shape, F32),
                V((NP * T, D), BF16),
                V((C, D, NP * T), BF16),
                V((D, 4 * D), BF16),
                V((H // 2, NP * T, 2 * LANES), BF16),
                V((NP, H // 2, 2 * T, T), BF16),
                V((X, XR, 4 * D // C), BF16),
                V((NP, D), F32),
                V((NP, 16, T), F32),
                V((C, NP * 16, D), BF16),
                V((NP, 16, T), F32),
                V((H // 2 // C, C, NP * T, 2 * LANES), BF16),
                V((H // 2 // C, NP * T, 2 * LANES), BF16),
                V((C, 3, NP, D), BF16),
                V((Z, R, LANES), BF16),
                V((Z, R, D - Y * LANES), BF16),
                V((3, Z, R, 2 * LANES), BF16),
                V((Y * C, 2, NP, LANES), F32),
                V((PARTS, 2, HR // 2, NC), BF16),
                V((PARTS, 2, X, HR // 2, NB), BF16),
                V((PARTS, 2, HR, NC), BF16),
                V((PARTS, HR, NC), BF16),
                V((PARTS, 2, X, HR, NB), BF16),
                V((PARTS, X, HR, NB), BF16),
                V((PARTS, Y - 1, HR, NB), BF16),
                V((PARTS, X - 1, HR, NB), BF16),
                V((PARTS, Z, R, NB), BF16),
                V((PARTS, Z - 1, R, NB), BF16),
                V((PARTS, Y * C, R, NB), BF16),
                V((Z, 8, LANES), F32),
                V((X * Y * C, 8, LANES), F32),
                dma((3,)),
                dma((2, 3, Z, 2)),
                dma((2, 3, 2, 2)),
                dma((2, 3, 2, 2)),
                dma((1, X, 2, 2)),
                dma((1, X, 2, 2)),
                dma((2, 1 + Y, 2)),
                dma((3, 2)),
                dma((2, H // 2 // C)),
                dma((Y * C, 2)),
                dma((PARTS, 2, 2)),
                dma((PARTS, 2, 2)),
                dma((PARTS, 2, 2)),
                dma((PARTS, 2, 2)),
                dma((PARTS, Y, 2)),
                dma((PARTS, X, 2)),
                dma((PARTS, Z, 2)),
                dma((PARTS, Y * C, 2)),
                dma((Z, 2)),
                dma((X * Y * C, 2)),
            ],
            compiler_params=pltpu.CompilerParams(collective_id=0, has_side_effects=True, vmem_limit_bytes=60 * 2**20),
        )(hidden, attn_weight, norm_gain, pos_bias, score_weight, pair_lengths, labels)
        scale = 1.0 / (jnp.sqrt(scalars[0] / (4.0 * D * D)) + EPS)
        return summed.astype(F32) * scale, scalars[1:]

    placed = (P(dp, cand, None, None), P(dp, None), P(), P(), P(), P(dp, cand), P(dp, cand))
    return jax.shard_map(shards, mesh=split, in_specs=placed, out_specs=(P(dp, None), P(dp)), check_vma=False)
```

```python
import functools

import jax
import jax.numpy as jnp
from jax import lax
from jax.experimental import pallas as pl
from jax.experimental.pallas import tpu as pltpu
from jax.sharding import Mesh
from jax.sharding import PartitionSpec as P

EPS = 1e-06
MESH = pl.DeviceIdType.MESH
F32, BF16 = jnp.float32, jnp.bfloat16
NEG = -1e30
PARTS = 3
LANES = 128


def dot(a, b, ca=1, cb=0):
    return lax.dot_general(a, b, (((ca,), (cb,)), ((), ())), preferred_element_type=F32)


def iota(shape, axis):
    return lax.broadcasted_iota(jnp.int32, shape, axis)


def step_kernel(dims, hid_in, wsh_in, gain, bias_in, sw, lens, labs, upd, out_s, hid, wsh, bias, norm, norm_t, w, qk, prob, grad,
                hsum, svec, avec, uvec, dqk, dsend, mixed, zc, za, zv, exb, a0, b0, a1, a1s, b1, b1s, a2, b2, zs, z3, ob, sqz, sq,
                lsem, zsem, xsem, xfsem, ysem, yfsem, dsem, psem, qsem, esem, a0sem, b0sem, a1sem, b1sem, a2sem, b2sem, z3sem, obsem,
                sqzsem, sqsem):
    X, Z, Y, C = dims
    QL, CL, T, D = hid.shape
    H = bias.shape[0]
    HP = H // 2
    HC = HP // C
    DC = D // C
    NP = QL * CL
    R = wsh.shape[0]
    XR = Z * R
    HR = XR // 2
    HQ = HR // 2
    ZH = Z // 2
    NC = 4 * D // PARTS // C
    NB = NC // Y
    x, z, y, c = (lax.axis_index(name) for name in ("x", "z", "y", "c"))
    other = 1 - c
    cand = y * C + c
    started = []

    def at_x(d):
        return {"x": lax.rem(x + d, X)}

    def at_z(d):
        return {"z": lax.rem(z + d, Z)}

    def at_y(d):
        return {"y": lax.rem(y + d, Y)}

    def at_cand(i):
        return {"y": lax.rem(y + i // C, Y), "c": lax.rem(c + i % C, C)}

    def put(src, dst, sems, to):
        copy = pltpu.make_async_remote_copy(src, dst, sems.at[0], sems.at[1], device_id=to, device_id_type=MESH)
        copy.start()
        started.append(copy)
        return copy

    def cols(n, width):
        return pl.ds(pl.multiple_of(n, LANES), width)

    loads = [pltpu.make_async_copy(src, dst, lsem.at[i]) for i, (src, dst) in enumerate(((hid_in, hid), (wsh_in, wsh), (bias_in, bias)))]
    for load in loads:
        load.start()

    near_x = [1] if X == 2 else [1, X - 1]
    near_y = [1] if Y == 2 else [1, Y - 1]
    first = [at_z(d) for d in range(1, Z)] + [at_x(d) for d in near_x] + [at_y(d) for d in near_y] + [{"c": other}]
    bar = pltpu.get_barrier_semaphore()
    for to in first:
        pl.semaphore_signal(bar, 1, device_id=to, device_id_type=MESH)

    def pair_len(p):
        return lens[p // CL, lax.rem(p, CL)]

    def normalise(p, carry):
        v = hid[p // CL, lax.rem(p, CL)].astype(F32)
        n = v * lax.rsqrt(jnp.mean(v * v, axis=1, keepdims=True) + EPS) * gain_row
        rows = pl.ds(pl.multiple_of(p * T, T), T)
        norm[rows, :] = n.astype(BF16)
        norm_t[c, :, cols(p * T, T)] = n.T.astype(BF16)
        live = iota((T, 1), 0) < pair_len(p)
        hsum[pl.ds(p, 1), :] = jnp.sum(jnp.where(live, v, 0.0), axis=0, keepdims=True)
        return carry

    gain_row, sw_row = gain[...].reshape(1, D), sw[...].reshape(1, D)
    loads[1].wait()
    pl.semaphore_wait(bar, len(first))

    def swap(ref, sem):
        return put(ref, ref, sem, {"c": other})


    AW = D - Y * LANES
    wide = {"c": LANES, "a": AW, 0: 2 * LANES, 1: 2 * LANES, 2: 2 * LANES}
    kinds = {0: ("c", "a"), 1: (0, 1, 2)}

    def wcols(g, core, kind, yy=0):
        base = (2 * g + core) * D
        return cols(base + (yy * LANES if kind == "c" else Y * LANES if kind == "a" else kind * 2 * LANES), wide[kind])

    def yrel(e):
        return lax.rem(y + e + Y, Y)

    def rows_of(d, lo=0, n=XR):
        return pl.ds(pl.multiple_of(lax.rem(x + d + X, X) * XR + lo, HR), n)

    zcopies, xcopies, xfcopies, ycopies, yfcopies, dcopies = {}, {}, {}, {}, {}, {}
    zbuf = {"c": zc, "a": za}

    def z_start(g):
        for i, kind in enumerate(kinds[g]):
            here = wcols(g, c, kind, y)
            for d in range(1, Z):
                zcopies[g, kind, d] = put(wsh.at[:, here], zbuf[kind].at[z], zsem.at[g, i, d], at_z(d))
            zbuf[kind][z] = wsh[:, here]

    z_near = [1] if Z == 2 else [1, 2, Z - 2, Z - 1]
    last = []

    def zv_start():
        here = cols((2 + c) * D, D)
        for i, d in enumerate(z_near):
            zcopies[1, d] = put(wsh.at[:, here], zv.at[z], zsem.at[1, 0, i], at_z(d))
        zv[z] = wsh[:, here]

    def zv_forward():
        for d in z_near:
            zcopies[1, d].wait_recv()
        if Z == 8:
            behind, ahead = lax.rem(z + Z - 2, Z), lax.rem(z + 2, Z)
            slot = jnp.where(c == 0, behind, ahead)
            far = jnp.where(c == 0, ahead, behind)
            last.append(put(zv.at[slot], zv.at[slot], zsem.at[1, 1, 0], {"z": far}))
            last.append(put(zv.at[behind], zv.at[behind], zsem.at[1, 1, 1], at_z(1)))
            last.append(put(zv.at[ahead], zv.at[ahead], zsem.at[1, 1, 2], at_z(Z - 1)))

    def zv_last():
        for copy in last:
            copy.wait_recv()

    def x_start(g, kind):
        i = kinds[g].index(kind)
        if g == 0:
            for d in range(1, Z):
                zcopies[g, kind, d].wait_recv()
        here = wcols(g, c, kind, y)
        got = zbuf[kind][...] if g == 0 else zv[:, :, kind * 2 * LANES : (kind + 1) * 2 * LANES]
        w[rows_of(0), here] = got.astype(F32).reshape(XR, wide[kind]).astype(BF16)
        own = w.at[rows_of(0), here]
        for j, d in enumerate(near_x):
            xcopies[g, kind, d] = put(own, own, xsem.at[g, i, j], at_x(d))

    def x_forward(g, kind):
        i = kinds[g].index(kind)
        for j, d in enumerate(near_x):
            xcopies[g, kind, d].wait_recv()
            if X == 4:
                half = w.at[rows_of(-d, 0 if d == 1 else HR, HR), wcols(g, c, kind, y)]
                xfcopies[g, kind, d] = put(half, half, xfsem.at[g, i, j], at_x(d))

    def x_last(g, kind):
        if X == 4:
            for d in near_x:
                xfcopies[g, kind, d].wait_recv()

    def y_start(g, d):
        blk = w.at[rows_of(d), wcols(g, c, "c", y)]
        for j, e in enumerate(near_y):
            ycopies[g, d, e] = put(blk, blk, ysem.at[g, d, j], at_y(e))

    def y_forward(g, d):
        for j, e in enumerate(near_y):
            ycopies[g, d, e].wait_recv()
            if Y == 4:
                half = w.at[rows_of(d, 0 if e == 1 else HR, HR), wcols(g, c, "c", yrel(-e))]
                yfcopies[g, d, e] = put(half, half, yfsem.at[g, d, j], at_y(e))

    def y_last(g):
        if Y == 4:
            for d in range(X):
                for e in near_y:
                    yfcopies[g, d, e].wait_recv()

    def hand_over(g, k, kind, yy=0):
        blk = w.at[:, wcols(g, c, kind, yy)]
        dcopies[g, k] = put(blk, blk, dsem.at[g, k], {"c": other})

    def hand_near(g):
        for e in near_y:
            hand_over(g, 1 + e, "c", yrel(e))

    def hand_last(g):
        y_last(g)
        if Y == 4:
            hand_over(g, 3, "c", yrel(2))

    def taken(g, keys):
        for k in keys:
            dcopies[g, k].wait_recv()

    def attend_a():
        taken(0, [0])
        lax.fori_loop(Y, HP, attend, 0)

    def attend_own():
        taken(0, [1])
        attend(y, 0)

    def attend_near():
        taken(0, [1 + e for e in near_y])
        lax.fori_loop(0, len(near_y), lambda i, carry: attend(lax.rem(y + 1 + i * (Y - 2), Y), carry), 0)

    def attend_far():
        if Y == 4:
            taken(0, [3])
            attend(yrel(2), 0)

    half_lane = iota((1, LANES), 1) < LANES // 2
    ones = [jnp.where(half_lane, 1.0, 0.0).astype(BF16), jnp.where(half_lane, 0.0, 1.0).astype(BF16)]

    def both(v):
        return jnp.concatenate([v * ones[0], v * ones[1]], axis=0)

    svec[...] = jnp.zeros_like(svec)

    def attend(h, carry):
        wqk = jnp.concatenate([w[:, cols(h * LANES, LANES)], w[:, cols(D + h * LANES, LANES)]], axis=1)
        qk[h] = dot(norm[...], wqk).astype(BF16)
        for p in range(NP):
            n_live = lens[p // CL, p % CL]
            live_key = iota((1, T), 1) < n_live
            live_row = iota((T, 1), 0) < n_live
            q2 = qk[h, p * T : (p + 1) * T, :LANES]
            k2 = qk[h, p * T : (p + 1) * T, LANES:]
            s = dot(both(q2), k2, 1, 1) + bias[pl.ds(2 * h, 2)].reshape(2 * T, T)
            s = jnp.where(live_key, s, NEG)
            e = jnp.exp(s - jnp.max(s, axis=1, keepdims=True))
            pr = (e * (1.0 / jnp.sum(e, axis=1, keepdims=True))).astype(BF16)
            prob[p, h] = pr
            for k in (0, 1):
                pk = jnp.where(live_row, pr[k * T : (k + 1) * T].astype(F32), 0.0)
                svec[p, pl.ds(2 * h + k, 1), :] = jnp.sum(pk, axis=0, keepdims=True)
        return carry

    z_start(0)
    zv_start()
    loads[0].wait()
    lax.fori_loop(0, NP, normalise, 0)
    norm_copy = swap(norm_t.at[c], psem.at[0])
    x_start(0, "c")
    y_start(0, 0)
    x_start(0, "a")
    x_forward(0, "c")
    for d in near_x:
        y_start(0, d)
    y_forward(0, 0)
    zv_forward()
    x_forward(0, "a")
    x_last(0, "c")
    if X == 4:
        y_start(0, 2)
    hand_over(0, 1, "c", y)
    for d in near_x:
        y_forward(0, d)
    x_last(0, "a")
    hand_over(0, 0, "a")
    zv_last()
    for k in kinds[1]:
        x_start(1, k)
    if X == 4:
        y_forward(0, 2)
    hand_near(0)
    loads[2].wait()
    attend_a()
    x_forward(1, 0)
    x_forward(1, 1)
    attend_own()
    hand_last(0)
    x_forward(1, 2)
    attend_near()
    for k in kinds[1]:
        x_last(1, k)
        hand_over(1, k, k)
    attend_far()
    for p in range(NP):
        avec[c, p * 16 : (p + 1) * 16, :] = dot(svec[p].astype(BF16), norm[p * T : (p + 1) * T, :]).astype(BF16)
    avec_copy = swap(avec.at[c], psem.at[1])
    taken(1, kinds[1])

    wv = w.at[:, 2 * D : 3 * D]
    wo = w.at[:, 3 * D : 4 * D]
    head_of = (iota((16, D), 1) // (D // H)) == iota((16, D), 0)
    prow = iota((NP, 1), 0)
    length, target = jnp.zeros((NP, 1), F32), jnp.zeros((NP, 1), F32)
    for p in range(NP):
        length = jnp.where(prow == p, lens[p // CL, p % CL].astype(F32), length)
        target = jnp.where(prow == p, labs[p // CL, p % CL].astype(F32), target)
    inv_len = 1.0 / length
    target = jnp.exp(target)

    zv = dot(avec[c], wv[...]).reshape(NP, 16, D)
    csum = jnp.sum(jnp.where(head_of[None], zv, 0.0), axis=1)
    pooled = hsum[...] * inv_len + dot((csum * inv_len).astype(BF16), wo[...])
    factor = lax.rsqrt(jnp.mean(pooled * pooled, axis=1, keepdims=True) + EPS)
    score = jnp.sum(pooled * factor * sw_row, axis=1, keepdims=True)

    exb[cand, 0] = jnp.broadcast_to(score, (NP, LANES))
    exb[cand, 1] = jnp.broadcast_to(target, (NP, LANES))
    ecopies = [put(exb.at[cand], exb.at[cand], esem.at[i], at_cand(i)) for i in range(1, Y * C)]

    along = jnp.sum(pooled * sw_row, axis=1, keepdims=True) * (1.0 / D)
    unit = (factor * sw_row - pooled * (factor * factor * factor * along)) * inv_len
    unit_b = unit.astype(BF16)
    cg = dot(unit_b, wo[...], 1, 1)
    for k, v in enumerate((csum.astype(BF16), unit_b, cg.astype(BF16))):
        mixed[c, k] = v
    mixed_copy = swap(mixed.at[c], psem.at[2])
    cexp = jnp.where(head_of[None], cg[:, None, :], 0.0).reshape(NP * 16, D).astype(BF16)
    tv = dot(cexp, wv[...], 1, 1).astype(BF16)
    for p in range(NP):
        uvec[p] = dot(tv[p * 16 : (p + 1) * 16], norm_t[c, :, p * T : (p + 1) * T])

    def listwise():
        for copy in ecopies:
            copy.wait_recv()
        scores, targets = exb[:, 0], exb[:, 1]
        query = iota((NP, LANES), 0) // CL

        def per_query(v, op, neutral):
            out = v
            for k in range(QL):
                out = jnp.where(query == k, op(jnp.where(query == k, v, neutral), axis=0, keepdims=True), out)
            return out

        highest = per_query(jnp.max(scores, axis=0), jnp.max, -jnp.inf)
        expsum = per_query(jnp.sum(jnp.exp(scores - highest[None]), axis=0), jnp.sum, 0.0)
        target_sum = per_query(jnp.sum(targets, axis=0), jnp.sum, 0.0)
        target_dot = per_query(jnp.sum(targets * scores, axis=0), jnp.sum, 0.0)
        losses = highest + jnp.log(expsum) - target_dot / target_sum
        for k in range(QL):
            out_s[1 + k] = jnp.max(losses[k * CL : k * CL + 1])
        grads = []
        for k in range(C):
            grads.append((jnp.exp(exb[y * C + k, 0] - highest) / expsum - exb[y * C + k, 1] / target_sum)[:, :1])
        return grads

    def keep(n, value):
        grad[:, :, n : n + value.shape[1]] = value.astype(BF16).reshape(X, XR, value.shape[1])

    def keep_outer(sgrad):
        avec_copy.wait_recv()
        mixed_copy.wait_recv()
        mine = cols(c * DC, DC)
        sums = jnp.concatenate([mixed[k, 0].astype(F32) for k in range(C)], axis=0).astype(BF16)
        outs = jnp.concatenate([mixed[k, 1, :, mine].astype(F32) * sgrad[k] for k in range(C)], axis=0).astype(BF16)
        keep(0, dot(sums, outs, 0, 0))
        lane_head = (c * DC + iota((16, DC), 1)) // (D // H) == iota((16, DC), 0)
        total = 0.0
        for k in range(C):
            rows = mixed[k, 2, :, mine].astype(F32) * sgrad[k]
            spread = jnp.where(lane_head[None], rows[:, None, :], 0.0).reshape(NP * 16, DC).astype(BF16)
            total += dot(avec[k], spread, 0, 0)
        keep(DC, total)

    def scale_norm(sgrad):
        norm_copy.wait_recv()
        norm_copy.wait_send()
        for k in range(C):
            for p in range(NP):
                v = norm_t[k, :, p * T : (p + 1) * T].astype(F32) * sgrad[k][p : p + 1]
                norm_t[k, :, p * T : (p + 1) * T] = v.astype(BF16)

    a0c, b0c, a1c, b1c, a2c, b2c, z3c, obc = {}, {}, {}, {}, {}, {}, {}, {}

    def lanes_of(t, yy=None):
        return pl.ds(t * NC, NC) if yy is None else cols(t * NC + yy * NB, NB)

    def reduce_1(t):
        if X == 4:
            far = lax.rem(x + 2, X)
            for j, d in enumerate(near_x):
                half = grad.at[far, j * HQ : (j + 1) * HQ, lanes_of(t)]
                a0c[t, j] = put(half, a0.at[t, j], a0sem.at[t, j], at_x(d))
        if Y == 4:
            for j, e in enumerate(near_y):
                half = grad.at[:, HR + j * HQ : HR + (j + 1) * HQ, lanes_of(t, yrel(2))]
                b0c[t, j] = put(half, b0.at[t, j], b0sem.at[t, j], at_y(e))

    def reduce_1b(t):
        for j, d in enumerate(near_x):
            ahead = lax.rem(x + d, X)
            if X == 4:
                a0c[t, j].wait_recv()
                part = pl.ds(j * HQ, HQ)
                grad[ahead, part, lanes_of(t)] = (grad[ahead, part, lanes_of(t)].astype(F32) + a0[t, j].astype(F32)).astype(BF16)
            a1c[t, j] = put(grad.at[ahead, :HR, lanes_of(t)], a1.at[t, j], a1sem.at[t, j], at_x(d))
        for j, e in enumerate(near_y):
            ahead = lanes_of(t, yrel(e))
            if Y == 4:
                b0c[t, j].wait_recv()
                part = pl.ds(HR + j * HQ, HQ)
                grad[:, part, ahead] = (grad[:, part, ahead].astype(F32) + b0[t, j].astype(F32)).astype(BF16)
            b1c[t, j] = put(grad.at[:, HR:, ahead], b1.at[t, j], b1sem.at[t, j], at_y(e))

    def reduce_2(t):
        total = grad[x, :HR, lanes_of(t)].astype(F32)
        for j in range(len(near_x)):
            a1c[t, j].wait_recv()
            total += a1[t, j].astype(F32)
        a1s[t] = total.astype(BF16)
        total = grad[:, HR:, lanes_of(t, y)].astype(F32)
        for j in range(len(near_y)):
            b1c[t, j].wait_recv()
            total += b1[t, j].astype(F32)
        b1s[t] = total.astype(BF16)
        for d in range(1, Y):
            a2c[t, d] = put(a1s.at[t, :, cols(lax.rem(y + d, Y) * NB, NB)], a2.at[t, d - 1], a2sem.at[t, d], at_y(d))
        for d in range(1, X):
            b2c[t, d] = put(b1s.at[t, lax.rem(x + d, X)], b2.at[t, d - 1], b2sem.at[t, d], at_x(d))

    def reduce_3(t):
        total = a1s[t, :, cols(y * NB, NB)].astype(F32)
        for d in range(1, Y):
            a2c[t, d].wait_recv()
            total += a2[t, d - 1].astype(F32)
        zs[t, :ZH] = total.reshape(ZH, R, NB).astype(BF16)
        total = b1s[t, x].astype(F32)
        for d in range(1, X):
            b2c[t, d].wait_recv()
            total += b2[t, d - 1].astype(F32)
        zs[t, ZH:] = total.reshape(ZH, R, NB).astype(BF16)
        for d in range(1, Z):
            z3c[t, d] = put(zs.at[t, lax.rem(z + d, Z)], z3.at[t, d - 1], z3sem.at[t, d], at_z(d))

    def reduce_4(t):
        total = zs[t, z].astype(F32)
        for d in range(1, Z):
            z3c[t, d].wait_recv()
            total += z3[t, d - 1].astype(F32)
        ob[t, cand] = total.astype(BF16)
        for i in range(1, Y * C):
            obc[t, i] = put(ob.at[t, cand], ob.at[t, cand], obsem.at[t, i], at_cand(i))

    def backward(h, out):
        for p in range(NP):
            n_live = lens[p // CL, p % CL]
            live_row = iota((T, 1), 0) < n_live
            rows = pl.ds(p * T, T)
            pr = prob[p, h].astype(F32).reshape(2, T, T)
            ds = []
            for k in (0, 1):
                pu = pr[k] * uvec[p, pl.ds(2 * h + k, 1), :]
                mean = jnp.sum(pu, axis=1, keepdims=True)
                ds.append(jnp.where(live_row, pu - pr[k] * mean, 0.0).astype(BF16))
            out[rows, :LANES] = dot(jnp.concatenate(ds, axis=1), both(qk[h, rows, LANES:])).astype(BF16)
            out[rows, LANES:] = dot(jnp.concatenate(ds, axis=0), both(qk[h, rows, :LANES]), 0, 0).astype(BF16)

    def dqk_copy(i):
        return pltpu.make_async_remote_copy(
            dsend.at[i], dqk.at[i, c], qsem.at[0, i], qsem.at[1, i], device_id={"c": other}, device_id_type=MESH
        )

    def for_partner(i, carry):
        backward(other * HC + i, dsend.at[i])
        dqk_copy(i).start()
        return carry

    def for_self(i, carry):
        backward(c * HC + i, dqk.at[i, c])
        return carry

    def keep_qk(i, carry):
        dqk_copy(i).wait()
        dw = dot(norm_t[0], dqk[i, 0]) + dot(norm_t[1], dqk[i, 1])
        grad[:, :, cols(2 * DC + i * 2 * LANES, 2 * LANES)] = dw.astype(BF16).reshape(X, XR, 2 * LANES)
        return carry

    lax.fori_loop(0, HC, for_partner, 0)
    lax.fori_loop(0, HC, for_self, 0)
    sgrad = listwise()
    keep_outer(sgrad)
    reduce_1(0)
    scale_norm(sgrad)
    keep_qk(0, 0)
    reduce_1(1)
    lax.fori_loop(1, HC, keep_qk, 0)
    reduce_1(2)
    reduce_1b(0)
    reduce_1b(1)
    reduce_1b(2)
    reduce_2(0)
    reduce_2(1)
    reduce_2(2)
    reduce_3(0)
    reduce_3(1)
    reduce_3(2)
    reduce_4(0)
    reduce_4(1)
    reduce_4(2)
    squares = jnp.zeros((R, NB), F32)
    for t in range(PARTS):
        v = ob[t, cand].astype(F32)
        squares += v * v
    squares = jnp.sum(jnp.sum(squares, axis=1, keepdims=True), axis=0, keepdims=True)
    sqz[z] = jnp.broadcast_to(squares, (8, LANES))
    zline = sqz.at[z, :1]
    zsq = [put(zline, zline, sqzsem.at[d], at_z(d)) for d in range(1, Z)]
    for copy in obc.values():
        copy.wait_recv()
    for t in range(PARTS):
        for k in range(Y * C):
            for m in range(NB // LANES):
                b, core = (t * NC + (k // C) * NB) // LANES + m, k % C
                outer = DC // LANES
                if b < outer:
                    n = 3 * D + core * DC + b * LANES
                elif b < 2 * outer:
                    n = 2 * D + core * DC + (b - outer) * LANES
                else:
                    n = (b - 2 * outer) % 2 * D + (core * HC + (b - 2 * outer) // 2) * LANES
                upd[:, n : n + LANES] = ob[t, k, :, m * LANES : (m + 1) * LANES]
    for copy in zsq:
        copy.wait_recv()
    me = x * Y * C + cand
    sq[me, :1] = jnp.sum(sqz[:, :1], axis=0)
    line = sq.at[me, :1]
    sqs = [put(line, line, sqsem.at[i], at_cand(i % (Y * C)) | at_x(i // (Y * C))) for i in range(1, X * Y * C)]
    for copy in started:
        if all(copy is not v for v in (*sqs, norm_copy)):
            copy.wait_send()
    for copy in sqs:
        copy.wait_recv()
    out_s[0] = jnp.max(jnp.sum(sq[:, :1], axis=0))
    for copy in sqs:
        copy.wait_send()


def finish_kernel(count, summed, scalars, update, loss):
    total = jnp.full((8, LANES), scalars[0], F32)
    scale = (1.0 / (jnp.sqrt(total * (1.0 / count)) + EPS))[:1, :1]
    update[...] = summed[...].astype(F32) * scale
    for k in range(loss.shape[0]):
        loss[k] = scalars[1 + k]


def solution(mesh):
    n_dp, n_cand = mesh.shape["dp"], mesh.shape["cand"]
    X, C = (4 if n_dp == 32 else 2), 2
    Z, Y = n_dp // X, n_cand // C
    split = Mesh(mesh.devices.reshape(X, Z, Y, C), ("x", "z", "y", "c"))
    dp, cand = ("x", "z"), ("y", "c")

    def shards(hidden, attn_weight, norm_gain, pos_bias, score_weight, pair_lengths, labels):
        QL, CL, T, D = hidden.shape
        H = pos_bias.shape[0]
        R = attn_weight.shape[0]
        NP, XR, NC = QL * CL, Z * R, 4 * D // PARTS // C
        HR, NB = XR // 2, NC // Y
        hbm = pl.BlockSpec(memory_space=pl.ANY)
        vmem, smem = pl.BlockSpec(memory_space=pltpu.VMEM), pl.BlockSpec(memory_space=pltpu.SMEM)
        dma = pltpu.SemaphoreType.DMA
        V = pltpu.VMEM
        summed, scalars = pl.pallas_call(
            functools.partial(step_kernel, (X, Z, Y, C)),
            out_shape=(
                jax.ShapeDtypeStruct((R, 4 * D), BF16),
                jax.ShapeDtypeStruct((1 + QL,), F32),
            ),
            in_specs=[hbm, hbm, vmem, hbm, vmem, smem, smem],
            out_specs=(vmem, smem),
            scratch_shapes=[
                V(hidden.shape, BF16),
                V(attn_weight.shape, BF16),
                V(pos_bias.shape, F32),
                V((NP * T, D), BF16),
                V((C, D, NP * T), BF16),
                V((D, 4 * D), BF16),
                V((H // 2, NP * T, 2 * LANES), BF16),
                V((NP, H // 2, 2 * T, T), BF16),
                V((X, XR, 4 * D // C), BF16),
                V((NP, D), F32),
                V((NP, 16, T), F32),
                V((C, NP * 16, D), BF16),
                V((NP, 16, T), F32),
                V((H // 2 // C, C, NP * T, 2 * LANES), BF16),
                V((H // 2 // C, NP * T, 2 * LANES), BF16),
                V((C, 3, NP, D), BF16),
                V((Z, R, LANES), BF16),
                V((Z, R, D - Y * LANES), BF16),
                V((Z, R, D), BF16),
                V((Y * C, 2, NP, LANES), F32),
                V((PARTS, 2, HR // 2, NC), BF16),
                V((PARTS, 2, X, HR // 2, NB), BF16),
                V((PARTS, 2, HR, NC), BF16),
                V((PARTS, HR, NC), BF16),
                V((PARTS, 2, X, HR, NB), BF16),
                V((PARTS, X, HR, NB), BF16),
                V((PARTS, Y - 1, HR, NB), BF16),
                V((PARTS, X - 1, HR, NB), BF16),
                V((PARTS, Z, R, NB), BF16),
                V((PARTS, Z - 1, R, NB), BF16),
                V((PARTS, Y * C, R, NB), BF16),
                V((Z, 8, LANES), F32),
                V((X * Y * C, 8, LANES), F32),
                dma((3,)),
                dma((2, 3, Z, 2)),
                dma((2, 3, 2, 2)),
                dma((2, 3, 2, 2)),
                dma((1, X, 2, 2)),
                dma((1, X, 2, 2)),
                dma((2, 1 + Y, 2)),
                dma((3, 2)),
                dma((2, H // 2 // C)),
                dma((Y * C, 2)),
                dma((PARTS, 2, 2)),
                dma((PARTS, 2, 2)),
                dma((PARTS, 2, 2)),
                dma((PARTS, 2, 2)),
                dma((PARTS, Y, 2)),
                dma((PARTS, X, 2)),
                dma((PARTS, Z, 2)),
                dma((PARTS, Y * C, 2)),
                dma((Z, 2)),
                dma((X * Y * C, 2)),
            ],
            compiler_params=pltpu.CompilerParams(collective_id=0, has_side_effects=True, vmem_limit_bytes=60 * 2**20),
        )(hidden, attn_weight, norm_gain, pos_bias, score_weight, pair_lengths, labels)
        return pl.pallas_call(
            functools.partial(finish_kernel, 4.0 * D * D),
            out_shape=(jax.ShapeDtypeStruct((R, 4 * D), F32), jax.ShapeDtypeStruct((QL,), F32)),
            in_specs=[vmem, smem],
            out_specs=(vmem, smem),
        )(summed, scalars)

    placed = (P(dp, cand, None, None), P(dp, None), P(), P(), P(), P(dp, cand), P(dp, cand))
    return jax.shard_map(shards, mesh=split, in_specs=placed, out_specs=(P(dp, None), P(dp)), check_vma=False)
```

```python
import functools

import jax
import jax.numpy as jnp
from jax import lax
from jax.experimental import pallas as pl
from jax.experimental.pallas import tpu as pltpu
from jax.sharding import Mesh
from jax.sharding import PartitionSpec as P

EPS = 1e-06
MESH = pl.DeviceIdType.MESH
F32, BF16 = jnp.float32, jnp.bfloat16
NEG = -1e30
PARTS = 3
LANES = 128


def dot(a, b, ca=1, cb=0):
    return lax.dot_general(a, b, (((ca,), (cb,)), ((), ())), preferred_element_type=F32)


def iota(shape, axis):
    return lax.broadcasted_iota(jnp.int32, shape, axis)


def step_kernel(dims, hid_in, wsh_in, gain, bias_in, sw, lens, labs, upd, out_s, hid, wsh, bias, norm, norm_t, w, qk, prob, grad,
                hsum, svec, avec, uvec, dqk, dsend, mixed, zc, za, zv, exb, a0, b0, a1, a1s, b1, b1s, a2, b2, zs, z3, ob, sqz, sq,
                lsem, zsem, xsem, xfsem, ysem, yfsem, dsem, psem, qsem, esem, a0sem, b0sem, a1sem, b1sem, a2sem, b2sem, z3sem, obsem,
                sqzsem, sqsem):
    X, Z, Y, C = dims
    QL, CL, T, D = hid.shape
    H = bias.shape[0]
    HP = H // 2
    HC = HP // C
    DC = D // C
    NP = QL * CL
    R = wsh.shape[0]
    XR = Z * R
    HR = XR // 2
    HQ = HR // 2
    ZH = Z // 2
    NC = 4 * D // PARTS // C
    NB = NC // Y
    x, z, y, c = (lax.axis_index(name) for name in ("x", "z", "y", "c"))
    other = 1 - c
    cand = y * C + c
    started = []

    def at_x(d):
        return {"x": lax.rem(x + d, X)}

    def at_z(d):
        return {"z": lax.rem(z + d, Z)}

    def at_y(d):
        return {"y": lax.rem(y + d, Y)}

    def at_cand(i):
        return {"y": lax.rem(y + i // C, Y), "c": lax.rem(c + i % C, C)}

    def put(src, dst, sems, to):
        copy = pltpu.make_async_remote_copy(src, dst, sems.at[0], sems.at[1], device_id=to, device_id_type=MESH)
        copy.start()
        started.append(copy)
        return copy

    def cols(n, width):
        return pl.ds(pl.multiple_of(n, LANES), width)

    loads = [pltpu.make_async_copy(src, dst, lsem.at[i]) for i, (src, dst) in enumerate(((hid_in, hid), (wsh_in, wsh), (bias_in, bias)))]
    for load in loads:
        load.start()

    near_x = [1] if X == 2 else [1, X - 1]
    near_y = [1] if Y == 2 else [1, Y - 1]
    first = [at_z(d) for d in range(1, Z)] + [at_x(d) for d in near_x] + [at_y(d) for d in near_y] + [{"c": other}]
    bar = pltpu.get_barrier_semaphore()
    for to in first:
        pl.semaphore_signal(bar, 1, device_id=to, device_id_type=MESH)

    def pair_len(p):
        return lens[p // CL, lax.rem(p, CL)]

    def normalise(p, carry):
        v = hid[p // CL, lax.rem(p, CL)].astype(F32)
        n = v * lax.rsqrt(jnp.mean(v * v, axis=1, keepdims=True) + EPS) * gain_row
        rows = pl.ds(pl.multiple_of(p * T, T), T)
        norm[rows, :] = n.astype(BF16)
        norm_t[c, :, cols(p * T, T)] = n.T.astype(BF16)
        live = iota((T, 1), 0) < pair_len(p)
        hsum[pl.ds(p, 1), :] = jnp.sum(jnp.where(live, v, 0.0), axis=0, keepdims=True)
        return carry

    gain_row, sw_row = gain[...].reshape(1, D), sw[...].reshape(1, D)
    loads[1].wait()
    pl.semaphore_wait(bar, len(first))

    def swap(ref, sem):
        return put(ref, ref, sem, {"c": other})


    AW = D - Y * LANES
    wide = {"c": LANES, "a": AW, 0: 2 * LANES, 1: 2 * LANES, 2: 2 * LANES}
    kinds = {0: ("c", "a"), 1: (0, 1, 2)}

    def wcols(g, core, kind, yy=0):
        base = (2 * g + core) * D
        return cols(base + (yy * LANES if kind == "c" else Y * LANES if kind == "a" else kind * 2 * LANES), wide[kind])

    def yrel(e):
        return lax.rem(y + e + Y, Y)

    def rows_of(d, lo=0, n=XR):
        return pl.ds(pl.multiple_of(lax.rem(x + d + X, X) * XR + lo, HR), n)

    zcopies, xcopies, xfcopies, ycopies, yfcopies, dcopies = {}, {}, {}, {}, {}, {}
    zbuf = {"c": zc, "a": za}

    def z_start(g):
        for i, kind in enumerate(kinds[g]):
            here = wcols(g, c, kind, y)
            for d in range(1, Z):
                zcopies[g, kind, d] = put(wsh.at[:, here], zbuf[kind].at[z], zsem.at[g, i, d], at_z(d))
            zbuf[kind][z] = wsh[:, here]

    z_near = [1] if Z == 2 else [1, 2, Z - 2, Z - 1]
    last = []

    def zv_start():
        here = cols((2 + c) * D, D)
        for i, d in enumerate(z_near):
            zcopies[1, d] = put(wsh.at[:, here], zv.at[z], zsem.at[1, 0, i], at_z(d))
        zv[z] = wsh[:, here]

    def zv_forward():
        for d in z_near:
            zcopies[1, d].wait_recv()
        if Z == 8:
            behind, ahead = lax.rem(z + Z - 2, Z), lax.rem(z + 2, Z)
            slot = jnp.where(c == 0, behind, ahead)
            far = jnp.where(c == 0, ahead, behind)
            last.append(put(zv.at[slot], zv.at[slot], zsem.at[1, 1, 0], {"z": far}))
            last.append(put(zv.at[behind], zv.at[behind], zsem.at[1, 1, 1], at_z(1)))
            last.append(put(zv.at[ahead], zv.at[ahead], zsem.at[1, 1, 2], at_z(Z - 1)))

    def zv_last():
        for copy in last:
            copy.wait_recv()

    def x_start(g, kind):
        i = kinds[g].index(kind)
        if g == 0:
            for d in range(1, Z):
                zcopies[g, kind, d].wait_recv()
        here = wcols(g, c, kind, y)
        got = zbuf[kind][...] if g == 0 else zv[:, :, kind * 2 * LANES : (kind + 1) * 2 * LANES]
        w[rows_of(0), here] = got.astype(F32).reshape(XR, wide[kind]).astype(BF16)
        own = w.at[rows_of(0), here]
        for j, d in enumerate(near_x):
            xcopies[g, kind, d] = put(own, own, xsem.at[g, i, j], at_x(d))

    def x_forward(g, kind):
        i = kinds[g].index(kind)
        for j, d in enumerate(near_x):
            xcopies[g, kind, d].wait_recv()
            if X == 4:
                half = w.at[rows_of(-d, 0 if d == 1 else HR, HR), wcols(g, c, kind, y)]
                xfcopies[g, kind, d] = put(half, half, xfsem.at[g, i, j], at_x(d))

    def x_last(g, kind):
        if X == 4:
            for d in near_x:
                xfcopies[g, kind, d].wait_recv()

    def y_start(g, d):
        blk = w.at[rows_of(d), wcols(g, c, "c", y)]
        for j, e in enumerate(near_y):
            ycopies[g, d, e] = put(blk, blk, ysem.at[g, d, j], at_y(e))

    def y_forward(g, d):
        for j, e in enumerate(near_y):
            ycopies[g, d, e].wait_recv()
            if Y == 4:
                half = w.at[rows_of(d, 0 if e == 1 else HR, HR), wcols(g, c, "c", yrel(-e))]
                yfcopies[g, d, e] = put(half, half, yfsem.at[g, d, j], at_y(e))

    def y_last(g):
        if Y == 4:
            for d in range(X):
                for e in near_y:
                    yfcopies[g, d, e].wait_recv()

    def hand_over(g, k, kind, yy=0):
        blk = w.at[:, wcols(g, c, kind, yy)]
        dcopies[g, k] = put(blk, blk, dsem.at[g, k], {"c": other})

    def hand_near(g):
        for e in near_y:
            hand_over(g, 1 + e, "c", yrel(e))

    def hand_last(g):
        y_last(g)
        if Y == 4:
            hand_over(g, 3, "c", yrel(2))

    def taken(g, keys):
        for k in keys:
            dcopies[g, k].wait_recv()

    def attend_a():
        taken(0, [0])
        lax.fori_loop(Y, HP, attend, 0)

    def attend_own():
        taken(0, [1])
        attend(y, 0)

    def attend_near():
        taken(0, [1 + e for e in near_y])
        lax.fori_loop(0, len(near_y), lambda i, carry: attend(lax.rem(y + 1 + i * (Y - 2), Y), carry), 0)

    def attend_far():
        if Y == 4:
            taken(0, [3])
            attend(yrel(2), 0)

    half_lane = iota((1, LANES), 1) < LANES // 2
    ones = [jnp.where(half_lane, 1.0, 0.0).astype(BF16), jnp.where(half_lane, 0.0, 1.0).astype(BF16)]

    def both(v):
        return jnp.concatenate([v * ones[0], v * ones[1]], axis=0)

    svec[...] = jnp.zeros_like(svec)

    def attend(h, carry):
        wqk = jnp.concatenate([w[:, cols(h * LANES, LANES)], w[:, cols(D + h * LANES, LANES)]], axis=1)
        qk[h] = dot(norm[...], wqk).astype(BF16)
        for p in range(NP):
            n_live = lens[p // CL, p % CL]
            live_key = iota((1, T), 1) < n_live
            live_row = iota((T, 1), 0) < n_live
            q2 = qk[h, p * T : (p + 1) * T, :LANES]
            k2 = qk[h, p * T : (p + 1) * T, LANES:]
            s = dot(both(q2), k2, 1, 1) + bias[pl.ds(2 * h, 2)].reshape(2 * T, T)
            s = jnp.where(live_key, s, NEG)
            e = jnp.exp(s - jnp.max(s, axis=1, keepdims=True))
            pr = (e * (1.0 / jnp.sum(e, axis=1, keepdims=True))).astype(BF16)
            prob[p, h] = pr
            for k in (0, 1):
                pk = jnp.where(live_row, pr[k * T : (k + 1) * T].astype(F32), 0.0)
                svec[p, pl.ds(2 * h + k, 1), :] = jnp.sum(pk, axis=0, keepdims=True)
        return carry

    z_start(0)
    zv_start()
    loads[0].wait()
    lax.fori_loop(0, NP, normalise, 0)
    norm_copy = swap(norm_t.at[c], psem.at[0])
    x_start(0, "c")
    y_start(0, 0)
    x_start(0, "a")
    x_forward(0, "c")
    for d in near_x:
        y_start(0, d)
    y_forward(0, 0)
    zv_forward()
    x_forward(0, "a")
    x_last(0, "c")
    if X == 4:
        y_start(0, 2)
    hand_over(0, 1, "c", y)
    for d in near_x:
        y_forward(0, d)
    x_last(0, "a")
    hand_over(0, 0, "a")
    zv_last()
    for k in kinds[1]:
        x_start(1, k)
    if X == 4:
        y_forward(0, 2)
    hand_near(0)
    loads[2].wait()
    attend_a()
    x_forward(1, 0)
    x_forward(1, 1)
    attend_own()
    hand_last(0)
    x_forward(1, 2)
    attend_near()
    for k in kinds[1]:
        x_last(1, k)
        hand_over(1, k, k)
    attend_far()
    for p in range(NP):
        avec[c, p * 16 : (p + 1) * 16, :] = dot(svec[p].astype(BF16), norm[p * T : (p + 1) * T, :]).astype(BF16)
    avec_copy = swap(avec.at[c], psem.at[1])
    taken(1, kinds[1])

    wv = w.at[:, 2 * D : 3 * D]
    wo = w.at[:, 3 * D : 4 * D]
    head_of = (iota((16, D), 1) // (D // H)) == iota((16, D), 0)
    prow = iota((NP, 1), 0)
    length, target = jnp.zeros((NP, 1), F32), jnp.zeros((NP, 1), F32)
    for p in range(NP):
        length = jnp.where(prow == p, lens[p // CL, p % CL].astype(F32), length)
        target = jnp.where(prow == p, labs[p // CL, p % CL].astype(F32), target)
    inv_len = 1.0 / length
    target = jnp.exp(target)

    zv = dot(avec[c], wv[...]).reshape(NP, 16, D)
    csum = jnp.sum(jnp.where(head_of[None], zv, 0.0), axis=1)
    pooled = hsum[...] * inv_len + dot((csum * inv_len).astype(BF16), wo[...])
    factor = lax.rsqrt(jnp.mean(pooled * pooled, axis=1, keepdims=True) + EPS)
    score = jnp.sum(pooled * factor * sw_row, axis=1, keepdims=True)

    exb[cand, 0] = jnp.broadcast_to(score, (NP, LANES))
    exb[cand, 1] = jnp.broadcast_to(target, (NP, LANES))
    ecopies = [put(exb.at[cand], exb.at[cand], esem.at[i], at_cand(i)) for i in range(1, Y * C)]

    along = jnp.sum(pooled * sw_row, axis=1, keepdims=True) * (1.0 / D)
    unit = (factor * sw_row - pooled * (factor * factor * factor * along)) * inv_len
    unit_b = unit.astype(BF16)
    cg = dot(unit_b, wo[...], 1, 1)
    for k, v in enumerate((csum.astype(BF16), unit_b, cg.astype(BF16))):
        mixed[c, k] = v
    mixed_copy = swap(mixed.at[c], psem.at[2])
    cexp = jnp.where(head_of[None], cg[:, None, :], 0.0).reshape(NP * 16, D).astype(BF16)
    tv = dot(cexp, wv[...], 1, 1).astype(BF16)
    for p in range(NP):
        uvec[p] = dot(tv[p * 16 : (p + 1) * 16], norm_t[c, :, p * T : (p + 1) * T])

    def listwise():
        for copy in ecopies:
            copy.wait_recv()
        scores, targets = exb[:, 0], exb[:, 1]
        query = iota((NP, LANES), 0) // CL

        def per_query(v, op, neutral):
            out = v
            for k in range(QL):
                out = jnp.where(query == k, op(jnp.where(query == k, v, neutral), axis=0, keepdims=True), out)
            return out

        highest = per_query(jnp.max(scores, axis=0), jnp.max, -jnp.inf)
        expsum = per_query(jnp.sum(jnp.exp(scores - highest[None]), axis=0), jnp.sum, 0.0)
        target_sum = per_query(jnp.sum(targets, axis=0), jnp.sum, 0.0)
        target_dot = per_query(jnp.sum(targets * scores, axis=0), jnp.sum, 0.0)
        losses = highest + jnp.log(expsum) - target_dot / target_sum
        for k in range(QL):
            out_s[1 + k] = jnp.max(losses[k * CL : k * CL + 1])
        grads = []
        for k in range(C):
            grads.append((jnp.exp(exb[y * C + k, 0] - highest) / expsum - exb[y * C + k, 1] / target_sum)[:, :1])
        return grads

    def keep(n, value):
        grad[:, :, n : n + value.shape[1]] = value.astype(BF16).reshape(X, XR, value.shape[1])

    def keep_outer(sgrad):
        avec_copy.wait_recv()
        mixed_copy.wait_recv()
        mine = cols(c * DC, DC)
        sums = jnp.concatenate([mixed[k, 0].astype(F32) for k in range(C)], axis=0).astype(BF16)
        outs = jnp.concatenate([mixed[k, 1, :, mine].astype(F32) * sgrad[k] for k in range(C)], axis=0).astype(BF16)
        keep(0, dot(sums, outs, 0, 0))
        lane_head = (c * DC + iota((16, DC), 1)) // (D // H) == iota((16, DC), 0)
        total = 0.0
        for k in range(C):
            rows = mixed[k, 2, :, mine].astype(F32) * sgrad[k]
            spread = jnp.where(lane_head[None], rows[:, None, :], 0.0).reshape(NP * 16, DC).astype(BF16)
            total += dot(avec[k], spread, 0, 0)
        keep(DC, total)

    def scale_norm(sgrad):
        norm_copy.wait_recv()
        norm_copy.wait_send()
        for k in range(C):
            for p in range(NP):
                v = norm_t[k, :, p * T : (p + 1) * T].astype(F32) * sgrad[k][p : p + 1]
                norm_t[k, :, p * T : (p + 1) * T] = v.astype(BF16)

    a0c, b0c, a1c, b1c, a2c, b2c, z3c, obc = {}, {}, {}, {}, {}, {}, {}, {}

    def lanes_of(t, yy=None):
        return pl.ds(t * NC, NC) if yy is None else cols(t * NC + yy * NB, NB)

    def reduce_1(t):
        if X == 4:
            far = lax.rem(x + 2, X)
            for j, d in enumerate(near_x):
                half = grad.at[far, j * HQ : (j + 1) * HQ, lanes_of(t)]
                a0c[t, j] = put(half, a0.at[t, j], a0sem.at[t, j], at_x(d))
        if Y == 4:
            for j, e in enumerate(near_y):
                half = grad.at[:, HR + j * HQ : HR + (j + 1) * HQ, lanes_of(t, yrel(2))]
                b0c[t, j] = put(half, b0.at[t, j], b0sem.at[t, j], at_y(e))

    def reduce_1b(t):
        for j, d in enumerate(near_x):
            ahead = lax.rem(x + d, X)
            if X == 4:
                a0c[t, j].wait_recv()
                part = pl.ds(j * HQ, HQ)
                grad[ahead, part, lanes_of(t)] = (grad[ahead, part, lanes_of(t)].astype(F32) + a0[t, j].astype(F32)).astype(BF16)
            a1c[t, j] = put(grad.at[ahead, :HR, lanes_of(t)], a1.at[t, j], a1sem.at[t, j], at_x(d))
        for j, e in enumerate(near_y):
            ahead = lanes_of(t, yrel(e))
            if Y == 4:
                b0c[t, j].wait_recv()
                part = pl.ds(HR + j * HQ, HQ)
                grad[:, part, ahead] = (grad[:, part, ahead].astype(F32) + b0[t, j].astype(F32)).astype(BF16)
            b1c[t, j] = put(grad.at[:, HR:, ahead], b1.at[t, j], b1sem.at[t, j], at_y(e))

    def reduce_2(t):
        total = grad[x, :HR, lanes_of(t)].astype(F32)
        for j in range(len(near_x)):
            a1c[t, j].wait_recv()
            total += a1[t, j].astype(F32)
        a1s[t] = total.astype(BF16)
        total = grad[:, HR:, lanes_of(t, y)].astype(F32)
        for j in range(len(near_y)):
            b1c[t, j].wait_recv()
            total += b1[t, j].astype(F32)
        b1s[t] = total.astype(BF16)
        for d in range(1, Y):
            a2c[t, d] = put(a1s.at[t, :, cols(lax.rem(y + d, Y) * NB, NB)], a2.at[t, d - 1], a2sem.at[t, d], at_y(d))
        for d in range(1, X):
            b2c[t, d] = put(b1s.at[t, lax.rem(x + d, X)], b2.at[t, d - 1], b2sem.at[t, d], at_x(d))

    def reduce_3(t):
        total = a1s[t, :, cols(y * NB, NB)].astype(F32)
        for d in range(1, Y):
            a2c[t, d].wait_recv()
            total += a2[t, d - 1].astype(F32)
        zs[t, :ZH] = total.reshape(ZH, R, NB).astype(BF16)
        total = b1s[t, x].astype(F32)
        for d in range(1, X):
            b2c[t, d].wait_recv()
            total += b2[t, d - 1].astype(F32)
        zs[t, ZH:] = total.reshape(ZH, R, NB).astype(BF16)
        for d in range(1, Z):
            z3c[t, d] = put(zs.at[t, lax.rem(z + d, Z)], z3.at[t, d - 1], z3sem.at[t, d], at_z(d))

    def reduce_4(t):
        total = zs[t, z].astype(F32)
        for d in range(1, Z):
            z3c[t, d].wait_recv()
            total += z3[t, d - 1].astype(F32)
        ob[t, cand] = total.astype(BF16)

    def spread(t):
        for i in range(1, Y * C):
            obc[t, i] = put(ob.at[t, cand], ob.at[t, cand], obsem.at[t, i], at_cand(i))

    def backward(h, out):
        for p in range(NP):
            n_live = lens[p // CL, p % CL]
            live_row = iota((T, 1), 0) < n_live
            rows = pl.ds(p * T, T)
            pr = prob[p, h].astype(F32).reshape(2, T, T)
            ds = []
            for k in (0, 1):
                pu = pr[k] * uvec[p, pl.ds(2 * h + k, 1), :]
                mean = jnp.sum(pu, axis=1, keepdims=True)
                ds.append(jnp.where(live_row, pu - pr[k] * mean, 0.0).astype(BF16))
            out[rows, :LANES] = dot(jnp.concatenate(ds, axis=1), both(qk[h, rows, LANES:])).astype(BF16)
            out[rows, LANES:] = dot(jnp.concatenate(ds, axis=0), both(qk[h, rows, :LANES]), 0, 0).astype(BF16)

    def dqk_copy(i):
        return pltpu.make_async_remote_copy(
            dsend.at[i], dqk.at[i, c], qsem.at[0, i], qsem.at[1, i], device_id={"c": other}, device_id_type=MESH
        )

    def for_partner(i, carry):
        backward(other * HC + i, dsend.at[i])
        dqk_copy(i).start()
        return carry

    def for_self(i, carry):
        backward(c * HC + i, dqk.at[i, c])
        return carry

    def keep_qk(i, carry):
        dqk_copy(i).wait()
        dw = dot(norm_t[0], dqk[i, 0]) + dot(norm_t[1], dqk[i, 1])
        grad[:, :, cols(2 * DC + i * 2 * LANES, 2 * LANES)] = dw.astype(BF16).reshape(X, XR, 2 * LANES)
        return carry

    lax.fori_loop(0, HC, for_partner, 0)
    lax.fori_loop(0, HC, for_self, 0)
    sgrad = listwise()
    keep_outer(sgrad)
    reduce_1(0)
    scale_norm(sgrad)
    keep_qk(0, 0)
    reduce_1(1)
    lax.fori_loop(1, HC, keep_qk, 0)
    reduce_1(2)
    reduce_1b(0)
    reduce_1b(1)
    reduce_1b(2)
    reduce_2(0)
    reduce_2(1)
    reduce_2(2)
    reduce_3(0)
    reduce_3(1)
    reduce_3(2)
    reduce_4(0)
    spread(0)
    reduce_4(1)
    spread(1)
    reduce_4(2)
    squares = jnp.zeros((R, NB), F32)
    for t in range(PARTS):
        v = ob[t, cand].astype(F32)
        squares += v * v
    squares = jnp.sum(jnp.sum(squares, axis=1, keepdims=True), axis=0, keepdims=True)
    sqz[z] = jnp.broadcast_to(squares, (8, LANES))
    zline = sqz.at[z, :1]
    zsq = [put(zline, zline, sqzsem.at[d], at_z(d)) for d in range(1, Z)]
    spread(PARTS - 1)

    def write_out():
        for copy in obc.values():
            copy.wait_recv()
        for t in range(PARTS):
            for k in range(Y * C):
                for m in range(NB // LANES):
                    b, core = (t * NC + (k // C) * NB) // LANES + m, k % C
                    outer = DC // LANES
                    if b < outer:
                        n = 3 * D + core * DC + b * LANES
                    elif b < 2 * outer:
                        n = 2 * D + core * DC + (b - outer) * LANES
                    else:
                        n = (b - 2 * outer) % 2 * D + (core * HC + (b - 2 * outer) // 2) * LANES
                    upd[:, n : n + LANES] = ob[t, k, :, m * LANES : (m + 1) * LANES]

    for copy in zsq:
        copy.wait_recv()
    me = x * Y * C + cand
    sq[me, :1] = jnp.sum(sqz[:, :1], axis=0)
    line = sq.at[me, :1]
    sqs = [put(line, line, sqsem.at[i], at_cand(i % (Y * C)) | at_x(i // (Y * C))) for i in range(1, X * Y * C)]
    write_out()
    for copy in started:
        if all(copy is not v for v in (*sqs, norm_copy)):
            copy.wait_send()
    for copy in sqs:
        copy.wait_recv()
    out_s[0] = jnp.max(jnp.sum(sq[:, :1], axis=0))
    for copy in sqs:
        copy.wait_send()


def finish_kernel(count, summed, scalars, update, loss):
    total = jnp.full((8, LANES), scalars[0], F32)
    scale = (1.0 / (jnp.sqrt(total * (1.0 / count)) + EPS))[:1, :1]
    update[...] = summed[...].astype(F32) * scale
    for k in range(loss.shape[0]):
        loss[k] = scalars[1 + k]


def solution(mesh):
    n_dp, n_cand = mesh.shape["dp"], mesh.shape["cand"]
    X, C = (4 if n_dp == 32 else 2), 2
    Z, Y = n_dp // X, n_cand // C
    split = Mesh(mesh.devices.reshape(X, Z, Y, C), ("x", "z", "y", "c"))
    dp, cand = ("x", "z"), ("y", "c")

    def shards(hidden, attn_weight, norm_gain, pos_bias, score_weight, pair_lengths, labels):
        QL, CL, T, D = hidden.shape
        H = pos_bias.shape[0]
        R = attn_weight.shape[0]
        NP, XR, NC = QL * CL, Z * R, 4 * D // PARTS // C
        HR, NB = XR // 2, NC // Y
        hbm = pl.BlockSpec(memory_space=pl.ANY)
        vmem, smem = pl.BlockSpec(memory_space=pltpu.VMEM), pl.BlockSpec(memory_space=pltpu.SMEM)
        dma = pltpu.SemaphoreType.DMA
        V = pltpu.VMEM
        summed, scalars = pl.pallas_call(
            functools.partial(step_kernel, (X, Z, Y, C)),
            out_shape=(
                jax.ShapeDtypeStruct((R, 4 * D), BF16),
                jax.ShapeDtypeStruct((1 + QL,), F32),
            ),
            in_specs=[hbm, hbm, vmem, hbm, vmem, smem, smem],
            out_specs=(vmem, smem),
            scratch_shapes=[
                V(hidden.shape, BF16),
                V(attn_weight.shape, BF16),
                V(pos_bias.shape, F32),
                V((NP * T, D), BF16),
                V((C, D, NP * T), BF16),
                V((D, 4 * D), BF16),
                V((H // 2, NP * T, 2 * LANES), BF16),
                V((NP, H // 2, 2 * T, T), BF16),
                V((X, XR, 4 * D // C), BF16),
                V((NP, D), F32),
                V((NP, 16, T), F32),
                V((C, NP * 16, D), BF16),
                V((NP, 16, T), F32),
                V((H // 2 // C, C, NP * T, 2 * LANES), BF16),
                V((H // 2 // C, NP * T, 2 * LANES), BF16),
                V((C, 3, NP, D), BF16),
                V((Z, R, LANES), BF16),
                V((Z, R, D - Y * LANES), BF16),
                V((Z, R, D), BF16),
                V((Y * C, 2, NP, LANES), F32),
                V((PARTS, 2, HR // 2, NC), BF16),
                V((PARTS, 2, X, HR // 2, NB), BF16),
                V((PARTS, 2, HR, NC), BF16),
                V((PARTS, HR, NC), BF16),
                V((PARTS, 2, X, HR, NB), BF16),
                V((PARTS, X, HR, NB), BF16),
                V((PARTS, Y - 1, HR, NB), BF16),
                V((PARTS, X - 1, HR, NB), BF16),
                V((PARTS, Z, R, NB), BF16),
                V((PARTS, Z - 1, R, NB), BF16),
                V((PARTS, Y * C, R, NB), BF16),
                V((Z, 8, LANES), F32),
                V((X * Y * C, 8, LANES), F32),
                dma((3,)),
                dma((2, 3, Z, 2)),
                dma((2, 3, 2, 2)),
                dma((2, 3, 2, 2)),
                dma((1, X, 2, 2)),
                dma((1, X, 2, 2)),
                dma((2, 1 + Y, 2)),
                dma((3, 2)),
                dma((2, H // 2 // C)),
                dma((Y * C, 2)),
                dma((PARTS, 2, 2)),
                dma((PARTS, 2, 2)),
                dma((PARTS, 2, 2)),
                dma((PARTS, 2, 2)),
                dma((PARTS, Y, 2)),
                dma((PARTS, X, 2)),
                dma((PARTS, Z, 2)),
                dma((PARTS, Y * C, 2)),
                dma((Z, 2)),
                dma((X * Y * C, 2)),
            ],
            compiler_params=pltpu.CompilerParams(collective_id=0, has_side_effects=True, vmem_limit_bytes=60 * 2**20),
        )(hidden, attn_weight, norm_gain, pos_bias, score_weight, pair_lengths, labels)
        return pl.pallas_call(
            functools.partial(finish_kernel, 4.0 * D * D),
            out_shape=(jax.ShapeDtypeStruct((R, 4 * D), F32), jax.ShapeDtypeStruct((QL,), F32)),
            in_specs=[vmem, smem],
            out_specs=(vmem, smem),
        )(summed, scalars)

    placed = (P(dp, cand, None, None), P(dp, None), P(), P(), P(), P(dp, cand), P(dp, cand))
    return jax.shard_map(shards, mesh=split, in_specs=placed, out_specs=(P(dp, None), P(dp)), check_vma=False)
```
